128 devices in a mesh: gx: 4 (over y), gy: 8 (over z, core), gz: 4 (over x).
Axes of the slice: x: 4, y: 4, z: 4, core: 2. Of those that a mesh axis runs over, the one named last changes fastest.
Arguments:
- params: float32 [12, 7168, 1536], P('gx', 'gy', 'gz'), may hold values from -100 to 100
- grads: bfloat16 [12, 7168, 1536], P('gx', 'gy', 'gz'), may hold values from -300 to 300
- row_state: float32 [12, 7168], P('gx', 'gy'), may hold values from 0.01 to 1
- col_state: float32 [12, 1536], P('gx', 'gz'), may hold values from 0.01 to 1
Outputs:
- new_params: float32 [12, 7168, 1536], P('gx', 'gy', 'gz')
- row_new: float32 [12, 7168], P('gx', 'gy')
- col_new: float32 [12, 1536], P('gx', 'gz')
- applied_step: float32 [12, 7168, 1536], P('gx', 'gy', 'gz')
- compute_copy: bfloat16 [12, 7168, 1536], P('gx', 'gy')
The draws below stay inside these ranges and needn't reach their ends.
All inputs are finite; a program needn't handle non-finite values.
Results may differ from the reference program's by a relative error of at most 0.0004.
Values may be sent and summed in bfloat16 or wider, within the bound.
A program may use at most 128 MiB of HBM per device.

```python
import math
import jax
import jax.numpy as jnp
from jax import lax

D = 7168
QR = 1536
LAY = 12


def draw_params(key, part):
    subkeys = jax.random.split(jax.random.fold_in(key, 17), 3)
    normal_part = jnp.clip(jax.random.normal(subkeys[0], (LAY, D, QR), jnp.float32), -6.0, 6.0)
    row_rise = jnp.arange(D, dtype=jnp.float32) / D
    col_rise = jnp.arange(QR, dtype=jnp.float32) / QR
    row_scale = 10.0 ** (0.5 * row_rise + 0.4 * jax.random.uniform(subkeys[1], (D,), jnp.float32) - 0.45)
    col_scale = 10.0 ** (0.5 * col_rise + 0.4 * jax.random.uniform(subkeys[2], (QR,), jnp.float32) - 0.45)
    weights = normal_part * row_scale[None, :, None] * col_scale[None, None, :]
    return weights.astype(jnp.float32)


def draw_grads(key, part):
    subkeys = jax.random.split(key, 3)
    normal_part = jnp.clip(jax.random.normal(subkeys[0], (LAY, D, QR), jnp.float32), -6.0, 6.0)
    row_rise = jnp.arange(D, dtype=jnp.float32) / D
    col_rise = jnp.arange(QR, dtype=jnp.float32) / QR
    layer_rise = jnp.arange(LAY, dtype=jnp.float32) / LAY
    row_scale = 10.0 ** (0.5 * row_rise + 0.5 * jax.random.uniform(subkeys[1], (D,), jnp.float32) - 0.5)
    col_scale = 10.0 ** (0.5 * col_rise + 0.5 * jax.random.uniform(subkeys[2], (QR,), jnp.float32) - 0.5)
    layer_scale = 10.0 ** (0.25 * layer_rise)
    gradient = normal_part * row_scale[None, :, None] * col_scale[None, None, :] * layer_scale[:, None, None]
    return gradient.astype(jnp.bfloat16)


def steps_of(own_key, dims, shards, least, top_value):
    def one(dim, shards_of):
        draws = jax.random.uniform(jax.random.fold_in(jax.random.fold_in(own_key, 6), dim), (shards_of,), jnp.float32, least / len(shards), top_value / len(shards))
        return jnp.repeat(jnp.exp(draws), dims[dim] // shards_of).reshape((-1,) + (1,) * (len(dims) - dim - 1))

    level = one(*shards[0])
    for cut in shards[1:]:
        level = level * one(*cut)
    return level


def setup_inputs(seed: int = 0) -> dict:
    streams_of = jax.random.split(jax.random.key(seed), 5)
    return {
        "params": draw_params(jax.random.fold_in(streams_of[4], 71), 0),
        "grads": draw_grads(jax.random.fold_in(streams_of[4], 71), 0),
        "row_state": jnp.clip(jnp.exp(math.log(1.0) - 4.6051702 * jax.random.uniform(streams_of[2], (LAY, D), jnp.float32) ** steps_of(streams_of[2], (LAY, D), ((0, 4), (1, 8)), -0.2, 0.2)), 0.01, 1.0),
        "col_state": jnp.clip(jnp.exp(math.log(1.0) - 4.6051702 * jax.random.uniform(streams_of[3], (LAY, QR), jnp.float32) ** steps_of(streams_of[3], (LAY, QR), ((0, 4), (1, 4)), -0.2, 0.2)), 0.01, 1.0),
    }


decay_rate = 0.842
tiny_term = 1e-30
step_share = 0.01
clip_limit = 1.0

def layer_factors(weights, gradient, row_old, col_old):
    grad_float = gradient.astype(jnp.float32)
    squares = grad_float * grad_float + tiny_term
    row_new = decay_rate * row_old + (1.0 - decay_rate) * lax.optimization_barrier(jnp.mean(squares, axis=1))
    col_new = decay_rate * col_old + (1.0 - decay_rate) * lax.optimization_barrier(jnp.mean(squares, axis=0))
    row_norm = row_new / jnp.mean(row_new)
    update = grad_float * lax.rsqrt(row_norm[:, None] * col_new[None, :])
    weight_scale = jnp.sqrt(jnp.mean(weights * weights))
    return (update, weight_scale, row_new, col_new)

def reference(params, grads, row_state, col_state):

    def measure_layer(operands):
        update, weight_scale, row_new, col_new = layer_factors(*operands)
        return (jnp.sum(update * update), weight_scale, row_new, col_new)
    update_sq, weight_scale, row_new, col_new = lax.map(measure_layer, (params, grads, row_state, col_state))
    root_mean = jnp.sqrt(jnp.sum(update_sq) / params.size)
    clip_factor = jnp.maximum(1.0, root_mean / clip_limit)

    def apply_layer(operands):
        weights, gradient, row_old, col_old, layer_scale = operands
        update = layer_factors(weights, gradient, row_old, col_old)[0]
        applied = layer_scale * update / clip_factor
        return (applied, weights - step_share * applied)
    applied_step, new_params = lax.map(apply_layer, (params, grads, row_state, col_state, weight_scale))
    return (new_params, row_new, col_new, applied_step, new_params.astype(jnp.bfloat16))
```

```python
import functools

import jax
import jax.numpy as jnp
from jax import lax
from jax.experimental import pallas as pl
from jax.experimental.pallas import tpu as pltpu
from jax.sharding import PartitionSpec as P

MESH = pl.DeviceIdType.MESH
F32 = jnp.float32
BF16 = jnp.bfloat16

decay_rate = 0.842
tiny_term = 1e-30
step_share = 0.01
clip_limit = 1.0

LAYERS = 3
ROWS = 896
COLS = 384
STEP = 64
TILES = STEP // 8
HALF = ROWS // 2


def lanes(shape):
    return lax.broadcasted_iota(jnp.int32, shape, len(shape) - 1)


def total(x):
    return jnp.sum(jnp.sum(x, axis=0, keepdims=True), axis=1, keepdims=True)


def lane_of(x, k):
    return jnp.sum(jnp.where(lanes(x.shape) == k, x, 0.0), axis=1, keepdims=True)


def pack_rows(lane_dense):
    sub = lax.broadcasted_iota(jnp.int32, (8, 128), 0)
    lane = lanes((8, 128))
    source = lax.broadcasted_iota(jnp.int32, (128, 128), 0)
    target = lanes((128, 128))
    packed = None
    for k in range(ROWS // 128):
        pick = (target == source // 8 + 16 * k).astype(F32)
        spread = [
            jnp.where(lane % 8 == sub, jnp.broadcast_to(lane_dense[l : l + 1, 128 * k : 128 * (k + 1)], (8, 128)), 0.0)
            for l in range(LAYERS)
        ]
        part = jnp.dot(
            jnp.concatenate(spread, axis=0), pick, preferred_element_type=F32, precision=lax.Precision.HIGHEST
        )
        packed = part if packed is None else packed + part
    return packed


def unpack_rows(packed):
    sub = lax.broadcasted_iota(jnp.int32, (8, 128), 0)
    lane = lanes((8, 128))
    source = lax.broadcasted_iota(jnp.int32, (128, 128), 0)
    target = lanes((128, 128))
    out = []
    for k in range(ROWS // 128):
        pick = (source == target // 8 + 16 * k).astype(F32)
        part = jnp.dot(packed, pick, preferred_element_type=F32, precision=lax.Precision.HIGHEST)
        out.append(
            [
                jnp.sum(jnp.where(lane % 8 == sub, part[8 * l : 8 * (l + 1)], 0.0), axis=0, keepdims=True)
                for l in range(LAYERS)
            ]
        )
    return out


def step_kernel(
    sizes,
    p_h, g_h, rs_h, cs_h,
    np_o, rn_o, cn_o, ap_o, cc_o,
    g_v, rs_v, cs_v, row_x, col_x, plane_x, stack_x, rrb,
    load_sem, row_s, row_r, col_s, col_r, plane_s, plane_r, stack_s, stack_r,
    right_s, right_r, left_s, left_r,
):
    nx, ny, nz = sizes
    gx, gy, gz = lax.axis_index("gx"), lax.axis_index("gy"), lax.axis_index("gz")
    right, left = lax.rem(gz + 1, nz), lax.rem(gz + nz - 1, nz)
    columns = COLS * nz
    rows_all = ROWS * ny

    loads = [pltpu.make_async_copy(g_h.at[l], g_v.at[l], load_sem.at[l]) for l in range(LAYERS)]
    loads += [
        pltpu.make_async_copy(rs_h, rs_v, load_sem.at[LAYERS]),
        pltpu.make_async_copy(cs_h, cs_v, load_sem.at[LAYERS + 1]),
    ]
    loads += [pltpu.make_async_copy(p_h.at[l], np_o.at[l], load_sem.at[LAYERS + 2 + l]) for l in range(LAYERS)]
    for load in loads:
        load.start()

    def plane_peer(i):
        return lax.rem(gy + i // nz, ny), lax.rem(gz + i % nz, nz)

    barrier = pltpu.get_barrier_semaphore()
    for i in range(1, ny * nz):
        y, z = plane_peer(i)
        pl.semaphore_signal(barrier, inc=1, device_id={"gx": gx, "gy": y, "gz": z}, device_id_type=MESH)
    for i in range(1, nx):
        x = lax.rem(gx + i, nx)
        pl.semaphore_signal(barrier, inc=1, device_id={"gx": x, "gy": gy, "gz": gz}, device_id_type=MESH)

    lane = lanes((8, 128))
    for l in range(LAYERS):
        loads[l].wait()

        def stats(i, carry, l=l):
            packed, col_acc = carry
            x = g_v[l, pl.ds(pl.multiple_of(i * STEP, STEP), STEP), :].astype(F32)
            sq = x * x
            row = jnp.sum(sq[:, 0:128] + sq[:, 128:256] + sq[:, 256:384], axis=1, keepdims=True)
            for k in range(TILES):
                packed = jnp.where(lane == i * TILES + k, row[8 * k : 8 * k + 8], packed)
                col_acc = col_acc + sq[8 * k : 8 * k + 8, :]
            return packed, col_acc

        packed, col_acc = lax.fori_loop(0, ROWS // STEP, stats, (jnp.zeros((8, 128), F32), jnp.zeros((8, COLS), F32)))
        row_x[gz, l] = packed
        col_x[gy, :, COLS * l : COLS * (l + 1)] = jnp.sum(col_acc, axis=0, keepdims=True)

    pl.semaphore_wait(barrier, ny * nz - 1 + nx - 1)
    exchange = []
    for i in range(1, nz):
        exchange.append(
            pltpu.make_async_remote_copy(
                row_x.at[gz], row_x.at[gz], row_s.at[i - 1], row_r.at[i - 1],
                device_id={"gx": gx, "gy": gy, "gz": lax.rem(gz + i, nz)}, device_id_type=MESH,
            )
        )
    for i in range(1, ny):
        exchange.append(
            pltpu.make_async_remote_copy(
                col_x.at[gy], col_x.at[gy], col_s.at[i - 1], col_r.at[i - 1],
                device_id={"gx": gx, "gy": lax.rem(gy + i, ny), "gz": gz}, device_id_type=MESH,
            )
        )
    for copy in exchange:
        copy.start()

    weight_sq = []
    for l in range(LAYERS):
        loads[LAYERS + 2 + l].wait()

        def weigh(i, acc, l=l):
            w = np_o[l, pl.ds(pl.multiple_of(i * STEP, STEP), STEP), :]
            sq = w * w
            for k in range(TILES):
                acc = acc + sq[8 * k : 8 * k + 8, :]
            return acc

        weight_sq.append(total(lax.fori_loop(0, ROWS // STEP, weigh, jnp.zeros((8, COLS), F32))))
    loads[LAYERS].wait()
    loads[LAYERS + 1].wait()
    row_old = pack_rows(rs_v[...])

    for copy in exchange:
        copy.wait_recv()
    row_new, row_inv, col_inv, update_sq, row_total = [], [], [], [], []
    for l in range(LAYERS):
        row_sum = row_x[0, l]
        for k in range(1, nz):
            row_sum = row_sum + row_x[k, l]
        new = decay_rate * row_old[8 * l : 8 * l + 8] + (1.0 - decay_rate) * (row_sum / columns + tiny_term)
        row_new.append(new)
        row_inv.append(lax.rsqrt(new))
        row_total.append(total(jnp.where(lane < ROWS // 8, new, 0.0)))
        col_sum = col_x[0, :, COLS * l : COLS * (l + 1)]
        for k in range(1, ny):
            col_sum = col_sum + col_x[k, :, COLS * l : COLS * (l + 1)]
        new = decay_rate * cs_v[l : l + 1, :] + (1.0 - decay_rate) * (col_sum / rows_all + tiny_term)
        cn_o[l : l + 1, :] = new
        col_inv.append(lax.rsqrt(new))

    for l in range(LAYERS):

        def updates(i, acc, l=l):
            rows = pl.ds(pl.multiple_of(i * STEP, STEP), STEP)
            x = g_v[l, rows, :].astype(F32)
            u = x * col_inv[l]
            sq = u * u
            y = sq[:, 0:128] + sq[:, 128:256] + sq[:, 256:384]
            for k in range(TILES):
                inv = jnp.sum(jnp.where(lane == i * TILES + k, row_inv[l], 0.0), axis=1, keepdims=True)
                inv = jnp.broadcast_to(inv, (8, 128))
                rrb[l, pl.ds(pl.multiple_of(i * STEP + 8 * k, 8), 8), :] = inv
                acc = acc + y[8 * k : 8 * k + 8] * (inv * inv)
            return acc

        update_sq.append(total(lax.fori_loop(0, ROWS // STEP, updates, jnp.zeros((8, 128), F32))))

    row1 = lanes((1, 128))
    payload = jnp.zeros((1, 128), F32)
    for l in range(LAYERS):
        payload = jnp.where(row1 == l, update_sq[l], payload)
        payload = jnp.where(row1 == LAYERS + l, weight_sq[l], payload)
        payload = jnp.where(row1 == 2 * LAYERS + l, row_total[l], payload)
    plane_x[gy * nz + gz] = payload
    plane = []
    for i in range(1, ny * nz):
        y, z = plane_peer(i)
        plane.append(
            pltpu.make_async_remote_copy(
                plane_x.at[gy * nz + gz], plane_x.at[gy * nz + gz], plane_s.at[i - 1], plane_r.at[i - 1],
                device_id={"gx": gx, "gy": y, "gz": z}, device_id_type=MESH,
            )
        )
    for copy in plane:
        copy.start()
    for copy in plane:
        copy.wait_recv()
    sums = plane_x[0]
    for i in range(1, ny * nz):
        sums = sums + plane_x[i]

    mean_row = [lane_of(sums, 2 * LAYERS + l) / (nz * rows_all) for l in range(LAYERS)]
    here = jnp.zeros((1, 1), F32)
    for l in range(LAYERS):
        here = here + mean_row[l] * lane_of(sums, l)
    stack_x[gx] = jnp.broadcast_to(here, (1, 128))
    stack = []
    for i in range(1, nx):
        stack.append(
            pltpu.make_async_remote_copy(
                stack_x.at[gx], stack_x.at[gx], stack_s.at[i - 1], stack_r.at[i - 1],
                device_id={"gx": lax.rem(gx + i, nx), "gy": gy, "gz": gz}, device_id_type=MESH,
            )
        )
    for copy in stack:
        copy.start()
    for copy in stack:
        copy.wait_recv()
    everything = stack_x[0]
    for i in range(1, nx):
        everything = everything + stack_x[i]
    entries = float(nx * LAYERS * rows_all * columns)
    clip = jnp.maximum(1.0, jnp.sqrt(everything / entries) / clip_limit)
    scale = []
    for l in range(LAYERS):
        weight = jnp.sqrt(lane_of(sums, LAYERS + l) / (rows_all * columns))
        scale.append(weight * jnp.sqrt(mean_row[l]) / clip)

    def apply(l, h):
        def some(i, carry):
            rows = pl.ds(pl.multiple_of(h * HALF + i * STEP, STEP), STEP)
            factor = rrb[l, rows, :] * scale[l]
            x = g_v[l, rows, :].astype(F32) * col_inv[l]
            w = np_o[l, rows, :]
            step = jnp.concatenate([x[:, 128 * k : 128 * k + 128] * factor for k in range(COLS // 128)], axis=1)
            new = w - step_share * step
            ap_o[l, rows, :] = step
            np_o[l, rows, :] = new
            cc_o[gz, l, rows, :] = new.astype(BF16)
            return carry

        lax.fori_loop(0, HALF // STEP, some, 0)

    def piece(owner, l, h):
        return cc_o.at[owner, l, pl.ds(h * HALF, HALF), :]

    def to_right(owner, l, h, n):
        return pltpu.make_async_remote_copy(
            piece(owner, l, h), piece(owner, l, h), right_s.at[n], right_r.at[n],
            device_id={"gx": gx, "gy": gy, "gz": right}, device_id_type=MESH,
        )

    def to_left(owner, l, h, n):
        return pltpu.make_async_remote_copy(
            piece(owner, l, h), piece(owner, l, h), left_s.at[n], left_r.at[n],
            device_id={"gx": gx, "gy": gy, "gz": left}, device_id_type=MESH,
        )

    rights, lefts = [], []
    for l in range(LAYERS):
        apply(l, 0)
        rights.append(to_right(gz, l, 0, l))
        rights[-1].start()
        apply(l, 1)
        lefts.append(to_left(gz, l, 1, l))
        lefts[-1].start()
    for l in range(LAYERS):
        rights.append(to_right(gz, l, 1, LAYERS + l))
        rights[-1].start()
        lefts.append(to_left(gz, l, 0, LAYERS + l))
        lefts[-1].start()

    new_rows = unpack_rows(jnp.concatenate(row_new, axis=0))
    for k in range(ROWS // 128):
        for l in range(LAYERS):
            rn_o[l : l + 1, 128 * k : 128 * (k + 1)] = new_rows[k][l]

    for l in range(LAYERS):
        rights[l].wait_recv()
        rights.append(to_right(left, l, 0, 2 * LAYERS + l))
        rights[-1].start()
        lefts[l].wait_recv()
        lefts.append(to_left(right, l, 1, 2 * LAYERS + l))
        lefts[-1].start()
    for n in range(LAYERS, 3 * LAYERS):
        rights[n].wait_recv()
        lefts[n].wait_recv()
    for copy in exchange + plane + stack + rights + lefts:
        copy.wait_send()


def write_kernel(np_v, rn_v, cn_v, ap_v, cc_v, np_h, rn_h, cn_h, ap_h, cc_h, sem):
    copies = []

    def put(source, target):
        copies.append(pltpu.make_async_copy(source, target, sem.at[len(copies)]))
        copies[-1].start()

    for l in range(LAYERS):
        for k in range(cc_v.shape[0]):
            put(cc_v.at[k, l], cc_h.at[l, :, pl.ds(COLS * k, COLS)])
        put(np_v.at[l], np_h.at[l])
        put(ap_v.at[l], ap_h.at[l])
    put(rn_v, rn_h)
    put(cn_v, cn_h)
    for copy in copies:
        copy.wait()


def solution(mesh):
    nx, ny, nz = (mesh.shape[a] for a in ("gx", "gy", "gz"))

    def body(params, grads, row_state, col_state):
        V = pltpu.VMEM
        sem = pltpu.SemaphoreType.DMA
        kept = pl.pallas_call(
            functools.partial(step_kernel, (nx, ny, nz)),
            out_shape=[
                V((LAYERS, ROWS, COLS), F32),
                V((LAYERS, ROWS), F32),
                V((LAYERS, COLS), F32),
                V((LAYERS, ROWS, COLS), F32),
                V((nz, LAYERS, ROWS, COLS), BF16),
            ],
            in_specs=[pl.BlockSpec(memory_space=pltpu.HBM)] * 4,
            out_specs=[pl.BlockSpec(memory_space=V)] * 5,
            scratch_shapes=[
                V((LAYERS, ROWS, COLS), BF16),
                V((LAYERS, ROWS), F32),
                V((LAYERS, COLS), F32),
                V((nz, LAYERS, 8, 128), F32),
                V((ny, 1, LAYERS * COLS), F32),
                V((ny * nz, 1, 128), F32),
                V((nx, 1, 128), F32),
                V((LAYERS, ROWS, 128), F32),
                sem((2 * LAYERS + 2,)),
                sem((nz - 1,)), sem((nz - 1,)),
                sem((ny - 1,)), sem((ny - 1,)),
                sem((ny * nz - 1,)), sem((ny * nz - 1,)),
                sem((nx - 1,)), sem((nx - 1,)),
                sem((3 * LAYERS,)), sem((3 * LAYERS,)),
                sem((3 * LAYERS,)), sem((3 * LAYERS,)),
            ],
            compiler_params=pltpu.CompilerParams(
                collective_id=0, has_side_effects=True, vmem_limit_bytes=16 * 2**20
            ),
        )(*[pltpu.with_memory_space_constraint(a, pltpu.HBM) for a in (params, grads, row_state, col_state)])
        return tuple(
            pl.pallas_call(
                write_kernel,
                out_shape=[
                    jax.ShapeDtypeStruct((LAYERS, ROWS, COLS), F32),
                    jax.ShapeDtypeStruct((LAYERS, ROWS), F32),
                    jax.ShapeDtypeStruct((LAYERS, COLS), F32),
                    jax.ShapeDtypeStruct((LAYERS, ROWS, COLS), F32),
                    jax.ShapeDtypeStruct((LAYERS, ROWS, nz * COLS), BF16),
                ],
                in_specs=[pl.BlockSpec(memory_space=V)] * 5,
                out_specs=[pl.BlockSpec(memory_space=pltpu.HBM)] * 5,
                scratch_shapes=[sem((LAYERS * (nz + 2) + 2,))],
                compiler_params=pltpu.CompilerParams(vmem_limit_bytes=2**20),
            )(*kept)
        )

    return jax.shard_map(
        body,
        mesh=mesh,
        in_specs=(P("gx", "gy", "gz"), P("gx", "gy", "gz"), P("gx", "gy"), P("gx", "gz")),
        out_specs=(
            P("gx", "gy", "gz"),
            P("gx", "gy"),
            P("gx", "gz"),
            P("gx", "gy", "gz"),
            P("gx", "gy", None),
        ),
        check_vma=False,
    )
```

```python
import functools

import jax
import jax.numpy as jnp
from jax import lax
from jax.experimental import pallas as pl
from jax.experimental.pallas import tpu as pltpu
from jax.sharding import PartitionSpec as P

MESH = pl.DeviceIdType.MESH
F32 = jnp.float32
BF16 = jnp.bfloat16

decay_rate = 0.842
tiny_term = 1e-30
step_share = 0.01
clip_limit = 1.0

LAYERS = 3
ROWS = 896
COLS = 384
STEP = 64
TILES = STEP // 8
HALF = ROWS // 2


def lanes(shape):
    return lax.broadcasted_iota(jnp.int32, shape, len(shape) - 1)


def total(x):
    return jnp.sum(jnp.sum(x, axis=0, keepdims=True), axis=1, keepdims=True)


def lane_of(x, k):
    return jnp.sum(jnp.where(lanes(x.shape) == k, x, 0.0), axis=1, keepdims=True)


def pack_rows(lane_dense):
    sub = lax.broadcasted_iota(jnp.int32, (8, 128), 0)
    lane = lanes((8, 128))
    source = lax.broadcasted_iota(jnp.int32, (128, 128), 0)
    target = lanes((128, 128))
    packed = None
    for k in range(ROWS // 128):
        pick = (target == source // 8 + 16 * k).astype(F32)
        spread = [
            jnp.where(lane % 8 == sub, jnp.broadcast_to(lane_dense[l : l + 1, 128 * k : 128 * (k + 1)], (8, 128)), 0.0)
            for l in range(LAYERS)
        ]
        part = jnp.dot(
            jnp.concatenate(spread, axis=0), pick, preferred_element_type=F32, precision=lax.Precision.HIGHEST
        )
        packed = part if packed is None else packed + part
    return packed


def unpack_rows(packed):
    sub = lax.broadcasted_iota(jnp.int32, (8, 128), 0)
    lane = lanes((8, 128))
    source = lax.broadcasted_iota(jnp.int32, (128, 128), 0)
    target = lanes((128, 128))
    out = []
    for k in range(ROWS // 128):
        pick = (source == target // 8 + 16 * k).astype(F32)
        part = jnp.dot(packed, pick, preferred_element_type=F32, precision=lax.Precision.HIGHEST)
        out.append(
            [
                jnp.sum(jnp.where(lane % 8 == sub, part[8 * l : 8 * (l + 1)], 0.0), axis=0, keepdims=True)
                for l in range(LAYERS)
            ]
        )
    return out


def step_kernel(
    sizes,
    p_h, g_h, rs_h, cs_h,
    np_o, rn_o, cn_o, ap_o, cc_o,
    g_v, rs_v, cs_v, row_x, col_x, all_x, row_inv, col_inv, rrb,
    load_sem, row_s, row_r, col_s, col_r, all_s, all_r,
    right_s, right_r, left_s, left_r,
):
    nx, ny, nz = sizes
    gx, gy, gz = lax.axis_index("gx"), lax.axis_index("gy"), lax.axis_index("gz")
    right, left = lax.rem(gz + 1, nz), lax.rem(gz + nz - 1, nz)
    columns = COLS * nz
    rows_all = ROWS * ny

    loads = [pltpu.make_async_copy(g_h.at[l], g_v.at[l], load_sem.at[l]) for l in range(LAYERS)]
    loads += [
        pltpu.make_async_copy(rs_h, rs_v, load_sem.at[LAYERS]),
        pltpu.make_async_copy(cs_h, cs_v, load_sem.at[LAYERS + 1]),
    ]
    loads += [pltpu.make_async_copy(p_h.at[l], np_o.at[l], load_sem.at[LAYERS + 2 + l]) for l in range(LAYERS)]
    for load in loads:
        load.start()

    xs = [lax.rem(gx + i, nx) for i in range(nx)]
    ys = [lax.rem(gy + i, ny) for i in range(ny)]
    zs = [lax.rem(gz + i, nz) for i in range(nz)]
    barrier = pltpu.get_barrier_semaphore()
    met = [(i, j, 0) for i in range(nx) for j in range(ny) if i or j] + [(0, 0, k) for k in range(1, nz)]
    for i, j, k in met:
        pl.semaphore_signal(barrier, inc=1, device_id={"gx": xs[i], "gy": ys[j], "gz": zs[k]}, device_id_type=MESH)

    lane = lanes((8, 128))

    def stats(l, carry):
        pltpu.make_async_copy(g_h.at[l], g_v.at[l], load_sem.at[l]).wait()
        packed = jnp.zeros((8, 128), F32)
        col_acc = jnp.zeros((8, COLS), F32)
        for t in range(ROWS // 16):
            x = g_v[l, 16 * t : 16 * t + 16, :].astype(F32)
            sq = x * x
            row = jnp.sum(sq[:, 0:128] + sq[:, 128:256] + sq[:, 256:384], axis=1, keepdims=True)
            packed = jnp.where(lane == 2 * t, row[0:8], packed)
            packed = jnp.where(lane == 2 * t + 1, row[8:16], packed)
            col_acc = col_acc + sq[0:8] + sq[8:16]
        row_x[gz, l] = packed
        col_x[gy, l] = jnp.sum(col_acc, axis=0, keepdims=True)
        return carry

    lax.fori_loop(0, LAYERS, stats, 0)

    pl.semaphore_wait(barrier, len(met))
    exchange = []
    for i in range(1, nz):
        exchange.append(
            pltpu.make_async_remote_copy(
                row_x.at[gz], row_x.at[gz], row_s.at[i - 1], row_r.at[i - 1],
                device_id={"gx": gx, "gy": gy, "gz": zs[i]}, device_id_type=MESH,
            )
        )
    for i in range(1, ny):
        exchange.append(
            pltpu.make_async_remote_copy(
                col_x.at[gy], col_x.at[gy], col_s.at[i - 1], col_r.at[i - 1],
                device_id={"gx": gx, "gy": ys[i], "gz": gz}, device_id_type=MESH,
            )
        )
    for copy in exchange:
        copy.start()

    row1 = lanes((1, 128))

    def weigh(l, payload):
        pltpu.make_async_copy(p_h.at[l], np_o.at[l], load_sem.at[LAYERS + 2 + l]).wait()

        def some(i, acc):
            w = np_o[l, pl.ds(pl.multiple_of(i * STEP, STEP), STEP), :]
            sq = w * w
            for k in range(TILES):
                acc = acc + sq[8 * k : 8 * k + 8, :]
            return acc

        squares = lax.fori_loop(0, ROWS // STEP, some, jnp.zeros((8, COLS), F32))
        return jnp.where(row1 == LAYERS + l, total(squares), payload)

    payload = lax.fori_loop(0, LAYERS, weigh, jnp.zeros((1, 128), F32))
    loads[LAYERS].wait()
    loads[LAYERS + 1].wait()
    row_old = pack_rows(rs_v[...])

    for copy in exchange:
        copy.wait_recv()
    row_new = []
    for l in range(LAYERS):
        row_sum = row_x[0, l]
        for k in range(1, nz):
            row_sum = row_sum + row_x[k, l]
        new = decay_rate * row_old[8 * l : 8 * l + 8] + (1.0 - decay_rate) * (row_sum / columns + tiny_term)
        row_new.append(new)
        row_inv[l] = lax.rsqrt(new)
        payload = jnp.where(row1 == 2 * LAYERS + l, total(jnp.where(lane < ROWS // 8, new, 0.0)), payload)
        col_sum = col_x[0, l]
        for k in range(1, ny):
            col_sum = col_sum + col_x[k, l]
        new = decay_rate * cs_v[l : l + 1, :] + (1.0 - decay_rate) * (col_sum / rows_all + tiny_term)
        cn_o[l : l + 1, :] = new
        col_inv[l] = lax.rsqrt(new)

    def updates(l, payload):
        acc = jnp.zeros((8, 128), F32)
        inv_packed = row_inv[l]
        inv_col = col_inv[l]
        for t in range(ROWS // 16):
            x = g_v[l, 16 * t : 16 * t + 16, :].astype(F32)
            u = x * inv_col
            sq = u * u
            y = sq[:, 0:128] + sq[:, 128:256] + sq[:, 256:384]
            for k in range(2):
                inv = jnp.sum(jnp.where(lane == 2 * t + k, inv_packed, 0.0), axis=1, keepdims=True)
                inv = jnp.broadcast_to(inv, (8, 128))
                rrb[l, 16 * t + 8 * k : 16 * t + 8 * k + 8, :] = inv
                acc = acc + y[8 * k : 8 * k + 8] * (inv * inv)
        return jnp.where(row1 == l, total(acc), payload)

    payload = lax.fori_loop(0, LAYERS, updates, payload)

    all_x[(gx * ny + gy) * nz + gz] = payload
    mine = all_x.at[(gx * ny + gy) * nz + gz]

    def far(at):
        return sum(min(a, n - a) for a, n in zip((at[0], at[1] // 2, at[2]), (nx, ny // 2, nz)))

    others = [(i, j, k) for i in range(nx) for j in range(ny) for k in range(nz) if i or j or k]
    for i, j, k in sorted(others, key=far, reverse=True):
        pltpu.make_async_remote_copy(
            mine, mine, all_s, all_r,
            device_id={"gx": xs[i], "gy": ys[j], "gz": zs[k]}, device_id_type=MESH,
        ).start()
    pltpu.make_async_copy(all_x.at[pl.ds(0, len(others))], all_x.at[pl.ds(0, len(others))], all_r).wait()
    everything = jnp.zeros((1, 1), F32)
    scale = [jnp.zeros((1, 1), F32)] * LAYERS
    for i in range(nx):
        sums = jnp.sum(all_x[i * ny * nz : (i + 1) * ny * nz], axis=0)
        for l in range(LAYERS):
            mean_row = lane_of(sums, 2 * LAYERS + l) / (nz * rows_all)
            everything = everything + mean_row * lane_of(sums, l)
            root = jnp.sqrt(lane_of(sums, LAYERS + l) / (rows_all * columns)) * jnp.sqrt(mean_row)
            scale[l] = jnp.where(gx == i, root, scale[l])
    entries = float(nx * LAYERS * rows_all * columns)
    clip = jnp.maximum(1.0, jnp.sqrt(everything / entries) / clip_limit)
    scale = [one / clip for one in scale]

    def apply(l, h):
        inv_col = col_inv[l]

        def some(i, carry):
            rows = pl.ds(pl.multiple_of(h * HALF + i * STEP, STEP), STEP)
            factor = rrb[l, rows, :] * scale[l]
            x = g_v[l, rows, :].astype(F32) * inv_col
            w = np_o[l, rows, :]
            step = jnp.concatenate([x[:, 128 * k : 128 * k + 128] * factor for k in range(COLS // 128)], axis=1)
            new = w - step_share * step
            ap_o[l, rows, :] = step
            np_o[l, rows, :] = new
            cc_o[gz, l, rows, :] = new.astype(BF16)
            return carry

        lax.fori_loop(0, HALF // STEP, some, 0)

    def piece(owner, l, h):
        return cc_o.at[owner, l, pl.ds(h * HALF, HALF), :]

    def to_right(owner, l, h, n):
        return pltpu.make_async_remote_copy(
            piece(owner, l, h), piece(owner, l, h), right_s.at[n], right_r.at[n],
            device_id={"gx": gx, "gy": gy, "gz": right}, device_id_type=MESH,
        )

    def to_left(owner, l, h, n):
        return pltpu.make_async_remote_copy(
            piece(owner, l, h), piece(owner, l, h), left_s.at[n], left_r.at[n],
            device_id={"gx": gx, "gy": gy, "gz": left}, device_id_type=MESH,
        )

    rights, lefts = [], []
    for l in range(LAYERS):
        apply(l, 0)
        rights.append(to_right(gz, l, 0, l))
        rights[-1].start()
        apply(l, 1)
        lefts.append(to_left(gz, l, 1, l))
        lefts[-1].start()
    for l in range(LAYERS):
        rights.append(to_right(gz, l, 1, LAYERS + l))
        rights[-1].start()
        lefts.append(to_left(gz, l, 0, LAYERS + l))
        lefts[-1].start()

    new_rows = unpack_rows(jnp.concatenate(row_new, axis=0))
    for k in range(ROWS // 128):
        for l in range(LAYERS):
            rn_o[l : l + 1, 128 * k : 128 * (k + 1)] = new_rows[k][l]

    for l in range(LAYERS):
        rights[l].wait_recv()
        rights.append(to_right(left, l, 0, 2 * LAYERS + l))
        rights[-1].start()
        lefts[l].wait_recv()
        lefts.append(to_left(right, l, 1, 2 * LAYERS + l))
        lefts[-1].start()
    for n in range(LAYERS, 3 * LAYERS):
        rights[n].wait_recv()
        lefts[n].wait_recv()
    for copy in exchange + rights + lefts:
        copy.wait_send()
    pltpu.make_async_copy(all_x.at[pl.ds(0, len(others))], all_x.at[pl.ds(0, len(others))], all_s).wait()


def write_kernel(np_v, rn_v, cn_v, ap_v, cc_v, np_h, rn_h, cn_h, ap_h, cc_h, sem):
    copies = []

    def put(source, target):
        copies.append(pltpu.make_async_copy(source, target, sem.at[len(copies)]))
        copies[-1].start()

    for l in range(LAYERS):
        for k in range(cc_v.shape[0]):
            put(cc_v.at[k, l], cc_h.at[l, :, pl.ds(COLS * k, COLS)])
        put(np_v.at[l], np_h.at[l])
        put(ap_v.at[l], ap_h.at[l])
    put(rn_v, rn_h)
    put(cn_v, cn_h)
    for copy in copies:
        copy.wait()


def solution(mesh):
    nx, ny, nz = (mesh.shape[a] for a in ("gx", "gy", "gz"))

    def body(params, grads, row_state, col_state):
        V = pltpu.VMEM
        sem = pltpu.SemaphoreType.DMA
        kept = pl.pallas_call(
            functools.partial(step_kernel, (nx, ny, nz)),
            out_shape=[
                V((LAYERS, ROWS, COLS), F32),
                V((LAYERS, ROWS), F32),
                V((LAYERS, COLS), F32),
                V((LAYERS, ROWS, COLS), F32),
                V((nz, LAYERS, ROWS, COLS), BF16),
            ],
            in_specs=[pl.BlockSpec(memory_space=pltpu.HBM)] * 4,
            out_specs=[pl.BlockSpec(memory_space=V)] * 5,
            scratch_shapes=[
                V((LAYERS, ROWS, COLS), BF16),
                V((LAYERS, ROWS), F32),
                V((LAYERS, COLS), F32),
                V((nz, LAYERS, 8, 128), F32),
                V((ny, LAYERS, 1, COLS), F32),
                V((nx * ny * nz, 1, 128), F32),
                V((LAYERS, 8, 128), F32),
                V((LAYERS, 1, COLS), F32),
                V((LAYERS, ROWS, 128), F32),
                sem((2 * LAYERS + 2,)),
                sem((nz - 1,)), sem((nz - 1,)),
                sem((ny - 1,)), sem((ny - 1,)),
                sem, sem,
                sem((3 * LAYERS,)), sem((3 * LAYERS,)),
                sem((3 * LAYERS,)), sem((3 * LAYERS,)),
            ],
            compiler_params=pltpu.CompilerParams(
                collective_id=0, has_side_effects=True, vmem_limit_bytes=16 * 2**20
            ),
        )(*[pltpu.with_memory_space_constraint(a, pltpu.HBM) for a in (params, grads, row_state, col_state)])
        return tuple(
            pl.pallas_call(
                write_kernel,
                out_shape=[
                    jax.ShapeDtypeStruct((LAYERS, ROWS, COLS), F32),
                    jax.ShapeDtypeStruct((LAYERS, ROWS), F32),
                    jax.ShapeDtypeStruct((LAYERS, COLS), F32),
                    jax.ShapeDtypeStruct((LAYERS, ROWS, COLS), F32),
                    jax.ShapeDtypeStruct((LAYERS, ROWS, nz * COLS), BF16),
                ],
                in_specs=[pl.BlockSpec(memory_space=V)] * 5,
                out_specs=[pl.BlockSpec(memory_space=pltpu.HBM)] * 5,
                scratch_shapes=[sem((LAYERS * (nz + 2) + 2,))],
                compiler_params=pltpu.CompilerParams(vmem_limit_bytes=2**20),
            )(*kept)
        )

    return jax.shard_map(
        body,
        mesh=mesh,
        in_specs=(P("gx", "gy", "gz"), P("gx", "gy", "gz"), P("gx", "gy"), P("gx", "gz")),
        out_specs=(
            P("gx", "gy", "gz"),
            P("gx", "gy"),
            P("gx", "gz"),
            P("gx", "gy", "gz"),
            P("gx", "gy", None),
        ),
        check_vma=False,
    )
```

```python
import functools

import jax
import jax.numpy as jnp
from jax import lax
from jax.experimental import pallas as pl
from jax.experimental.pallas import tpu as pltpu
from jax.sharding import PartitionSpec as P

MESH = pl.DeviceIdType.MESH
F32 = jnp.float32
BF16 = jnp.bfloat16

decay_rate = 0.842
tiny_term = 1e-30
step_share = 0.01
clip_limit = 1.0

LAYERS = 3
ROWS = 896
COLS = 384
STEP = 32
TILES = STEP // 8
PIECE = ROWS // 4
PIECES = 2 * LAYERS
EARLY = (0, 6)


def place(kind, n):
    return n // 2, (2 * kind + n % 2) * PIECE


def lanes(shape):
    return lax.broadcasted_iota(jnp.int32, shape, len(shape) - 1)


def total(x):
    return jnp.sum(jnp.sum(x, axis=0, keepdims=True), axis=1, keepdims=True)


def lane_of(x, k):
    return jnp.sum(jnp.where(lanes(x.shape) == k, x, 0.0), axis=1, keepdims=True)


def pack_rows(lane_dense):
    sub = lax.broadcasted_iota(jnp.int32, (8, 128), 0)
    lane = lanes((8, 128))
    source = lax.broadcasted_iota(jnp.int32, (128, 128), 0)
    target = lanes((128, 128))
    packed = None
    for k in range(ROWS // 128):
        pick = (target == source // 8 + 16 * k).astype(F32)
        spread = [
            jnp.where(lane % 8 == sub, jnp.broadcast_to(lane_dense[l : l + 1, 128 * k : 128 * (k + 1)], (8, 128)), 0.0)
            for l in range(LAYERS)
        ]
        part = jnp.dot(
            jnp.concatenate(spread, axis=0), pick, preferred_element_type=F32, precision=lax.Precision.HIGHEST
        )
        packed = part if packed is None else packed + part
    return packed


def unpack_rows(packed):
    sub = lax.broadcasted_iota(jnp.int32, (8, 128), 0)
    lane = lanes((8, 128))
    source = lax.broadcasted_iota(jnp.int32, (128, 128), 0)
    target = lanes((128, 128))
    out = []
    for k in range(ROWS // 128):
        pick = (source == target // 8 + 16 * k).astype(F32)
        part = jnp.dot(packed, pick, preferred_element_type=F32, precision=lax.Precision.HIGHEST)
        out.append(
            [
                jnp.sum(jnp.where(lane % 8 == sub, part[8 * l : 8 * (l + 1)], 0.0), axis=0, keepdims=True)
                for l in range(LAYERS)
            ]
        )
    return out


def step_kernel(
    sizes,
    p_h, g_h, rs_h, cs_h,
    np_o, rn_o, cn_o, ap_o, cc_o,
    g_v, rs_v, cs_v, row_x, col_x, all_x, row_inv, col_inv, rrb,
    load_sem, row_s, row_r, col_s, col_r, all_s, all_r,
    right_s, right_r, left_s, left_r,
):
    nx, ny, nz = sizes
    gx, gy, gz = lax.axis_index("gx"), lax.axis_index("gy"), lax.axis_index("gz")
    right, left = lax.rem(gz + 1, nz), lax.rem(gz + nz - 1, nz)
    columns = COLS * nz
    rows_all = ROWS * ny

    loads = [pltpu.make_async_copy(g_h.at[l], g_v.at[l], load_sem.at[l]) for l in range(LAYERS)]
    loads += [
        pltpu.make_async_copy(rs_h, rs_v, load_sem.at[LAYERS]),
        pltpu.make_async_copy(cs_h, cs_v, load_sem.at[LAYERS + 1]),
    ]
    loads += [pltpu.make_async_copy(p_h.at[l], np_o.at[l], load_sem.at[LAYERS + 2 + l]) for l in range(LAYERS)]
    for load in loads:
        load.start()

    xs = [lax.rem(gx + i, nx) for i in range(nx)]
    ys = [lax.rem(gy + i, ny) for i in range(ny)]
    zs = [lax.rem(gz + i, nz) for i in range(nz)]
    barrier = pltpu.get_barrier_semaphore()
    met = [(i, j, 0) for i in range(nx) for j in range(ny) if i or j] + [(0, 0, k) for k in range(1, nz)]
    for i, j, k in met:
        pl.semaphore_signal(barrier, inc=1, device_id={"gx": xs[i], "gy": ys[j], "gz": zs[k]}, device_id_type=MESH)

    lane = lanes((8, 128))

    def stats(l, carry):
        pltpu.make_async_copy(g_h.at[l], g_v.at[l], load_sem.at[l]).wait()
        packed = jnp.zeros((8, 128), F32)
        col_acc = jnp.zeros((8, COLS), F32)
        for t in range(ROWS // 16):
            x = g_v[l, 16 * t : 16 * t + 16, :].astype(F32)
            sq = x * x
            row = jnp.sum(sq[:, 0:128] + sq[:, 128:256] + sq[:, 256:384], axis=1, keepdims=True)
            packed = jnp.where(lane == 2 * t, row[0:8], packed)
            packed = jnp.where(lane == 2 * t + 1, row[8:16], packed)
            col_acc = col_acc + sq[0:8] + sq[8:16]
        row_x[gz, l] = packed
        col_x[gy, l] = jnp.sum(col_acc, axis=0, keepdims=True)
        return carry

    lax.fori_loop(0, LAYERS, stats, 0)

    pl.semaphore_wait(barrier, len(met))
    exchange = []
    for i in range(1, nz):
        exchange.append(
            pltpu.make_async_remote_copy(
                row_x.at[gz], row_x.at[gz], row_s.at[i - 1], row_r.at[i - 1],
                device_id={"gx": gx, "gy": gy, "gz": zs[i]}, device_id_type=MESH,
            )
        )
    for i in range(1, ny):
        exchange.append(
            pltpu.make_async_remote_copy(
                col_x.at[gy], col_x.at[gy], col_s.at[i - 1], col_r.at[i - 1],
                device_id={"gx": gx, "gy": ys[i], "gz": gz}, device_id_type=MESH,
            )
        )
    for copy in exchange:
        copy.start()

    row1 = lanes((1, 128))

    def weigh(l, payload):
        pltpu.make_async_copy(p_h.at[l], np_o.at[l], load_sem.at[LAYERS + 2 + l]).wait()

        def some(i, acc):
            w = np_o[l, pl.ds(pl.multiple_of(i * STEP, STEP), STEP), :]
            sq = w * w
            for k in range(TILES):
                acc = acc + sq[8 * k : 8 * k + 8, :]
            return acc

        squares = lax.fori_loop(0, ROWS // STEP, some, jnp.zeros((8, COLS), F32))
        return jnp.where(row1 == LAYERS + l, total(squares), payload)

    payload = lax.fori_loop(0, LAYERS, weigh, jnp.zeros((1, 128), F32))
    loads[LAYERS].wait()
    loads[LAYERS + 1].wait()
    row_old = pack_rows(rs_v[...])

    for copy in exchange:
        copy.wait_recv()
    row_new = []
    for l in range(LAYERS):
        row_sum = row_x[0, l]
        for k in range(1, nz):
            row_sum = row_sum + row_x[k, l]
        new = decay_rate * row_old[8 * l : 8 * l + 8] + (1.0 - decay_rate) * (row_sum / columns + tiny_term)
        row_new.append(new)
        row_inv[l] = lax.rsqrt(new)
        payload = jnp.where(row1 == 2 * LAYERS + l, total(jnp.where(lane < ROWS // 8, new, 0.0)), payload)
        col_sum = col_x[0, l]
        for k in range(1, ny):
            col_sum = col_sum + col_x[k, l]
        new = decay_rate * cs_v[l : l + 1, :] + (1.0 - decay_rate) * (col_sum / rows_all + tiny_term)
        cn_o[l : l + 1, :] = new
        col_inv[l] = lax.rsqrt(new)

    def updates(l, payload):
        acc = jnp.zeros((8, 128), F32)
        inv_packed = row_inv[l]
        inv_col = col_inv[l]
        for t in range(ROWS // 16):
            x = g_v[l, 16 * t : 16 * t + 16, :].astype(F32)
            u = x * inv_col
            sq = u * u
            y = sq[:, 0:128] + sq[:, 128:256] + sq[:, 256:384]
            for k in range(2):
                inv = jnp.sum(jnp.where(lane == 2 * t + k, inv_packed, 0.0), axis=1, keepdims=True)
                inv = jnp.broadcast_to(inv, (8, 128))
                rrb[l, 16 * t + 8 * k : 16 * t + 8 * k + 8, :] = inv
                acc = acc + y[8 * k : 8 * k + 8] * (inv * inv)
        return jnp.where(row1 == l, total(acc), payload)

    payload = lax.fori_loop(0, LAYERS, updates, payload)

    all_x[(gx * ny + gy) * nz + gz] = payload
    mine = all_x.at[(gx * ny + gy) * nz + gz]

    def far(at):
        return sum(min(a, n - a) for a, n in zip((at[0], at[1] // 2, at[2]), (nx, ny // 2, nz)))

    others = [(i, j, k) for i in range(nx) for j in range(ny) for k in range(nz) if i or j or k]
    for i, j, k in sorted(others, key=far, reverse=True):
        pltpu.make_async_remote_copy(
            mine, mine, all_s, all_r,
            device_id={"gx": xs[i], "gy": ys[j], "gz": zs[k]}, device_id_type=MESH,
        ).start()
    pltpu.make_async_copy(all_x.at[pl.ds(0, len(others))], all_x.at[pl.ds(0, len(others))], all_r).wait()
    everything = jnp.zeros((1, 1), F32)
    scale = [jnp.zeros((1, 1), F32)] * LAYERS
    for i in range(nx):
        sums = jnp.sum(all_x[i * ny * nz : (i + 1) * ny * nz], axis=0)
        for l in range(LAYERS):
            mean_row = lane_of(sums, 2 * LAYERS + l) / (nz * rows_all)
            everything = everything + mean_row * lane_of(sums, l)
            root = jnp.sqrt(lane_of(sums, LAYERS + l) / (rows_all * columns)) * jnp.sqrt(mean_row)
            scale[l] = jnp.where(gx == i, root, scale[l])
    entries = float(nx * LAYERS * rows_all * columns)
    clip = jnp.maximum(1.0, jnp.sqrt(everything / entries) / clip_limit)
    scale = [one / clip for one in scale]

    def apply(l, first):
        inv_col = col_inv[l]

        def some(i, carry):
            rows = pl.ds(pl.multiple_of(first + i * STEP, STEP), STEP)
            factor = rrb[l, rows, :] * scale[l]
            x = g_v[l, rows, :].astype(F32) * inv_col
            w = np_o[l, rows, :]
            step = jnp.concatenate([x[:, 128 * k : 128 * k + 128] * factor for k in range(COLS // 128)], axis=1)
            new = w - step_share * step
            ap_o[l, rows, :] = step
            np_o[l, rows, :] = new
            cc_o[gz, l, rows, :] = new.astype(BF16)
            return carry

        lax.fori_loop(0, PIECE // STEP, some, 0)

    def send(owner, kind, n, way, number):
        l, first = place(kind, n)
        piece = cc_o.at[owner, l, pl.ds(first, PIECE), :]
        return pltpu.make_async_remote_copy(
            piece, piece, (right_s, left_s)[way].at[number], (right_r, left_r)[way].at[number],
            device_id={"gx": gx, "gy": gy, "gz": (right, left)[way]}, device_id_type=MESH,
        )

    core = lax.rem(gy, 2)
    own = ([send(gz, 0, n, 0, n) for n in range(PIECES)], [send(gz, 1, n, 1, n) for n in range(PIECES)])
    last = ([send(gz, 1, n, 0, PIECES + n) for n in range(PIECES)], [send(gz, 0, n, 1, PIECES + n) for n in range(PIECES)])
    on = (
        [send(left, 0, n, 0, 2 * PIECES + n) for n in range(PIECES)],
        [send(right, 1, n, 1, 2 * PIECES + n) for n in range(PIECES)],
    )
    for n in range(PIECES):
        for way in range(2):
            apply(*place(way, n))
            own[way][n].start()

    def extra(do):
        for n in range(min(EARLY)):
            for way in range(2):
                do(last[way][n])

        @pl.when(core == (0 if EARLY[0] > EARLY[1] else 1))
        def _():
            for n in range(min(EARLY), max(EARLY)):
                for way in range(2):
                    do(last[way][n])

    extra(lambda copy: copy.start())
    new_rows = unpack_rows(jnp.concatenate(row_new, axis=0))
    for k in range(ROWS // 128):
        for l in range(LAYERS):
            rn_o[l : l + 1, 128 * k : 128 * (k + 1)] = new_rows[k][l]

    for n in range(PIECES):
        for way in range(2):
            own[way][n].wait_recv()
            on[way][n].start()
    for way in range(2):
        for n in range(PIECES):
            on[way][n].wait_recv()
    extra(lambda copy: copy.wait_recv())
    for copy in exchange + own[0] + own[1] + on[0] + on[1]:
        copy.wait_send()
    extra(lambda copy: copy.wait_send())
    pltpu.make_async_copy(all_x.at[pl.ds(0, len(others))], all_x.at[pl.ds(0, len(others))], all_s).wait()


def rest(core, early, late):
    for n in range(PIECES):
        for way in range(2):
            if n < min(EARLY):
                early(way, n)
            elif n >= max(EARLY):
                late(way, n)

    ahead = 0 if EARLY[0] > EARLY[1] else 1
    for mine, do in ((ahead, early), (1 - ahead, late)):

        @pl.when(core == mine)
        def _(do=do):
            for n in range(min(EARLY), max(EARLY)):
                for way in range(2):
                    do(way, n)


def columns_of(owner):
    return pl.ds(pl.multiple_of(owner * COLS, COLS), COLS)


def rest_kernel(nz, cc_v, after_h, late_o, right_s, right_r, left_s, left_r):
    gx, gy, gz = lax.axis_index("gx"), lax.axis_index("gy"), lax.axis_index("gz")
    right, left = lax.rem(gz + 1, nz), lax.rem(gz + nz - 1, nz)
    barrier = pltpu.get_barrier_semaphore()
    for z in (right, left):
        pl.semaphore_signal(barrier, inc=1, device_id={"gx": gx, "gy": gy, "gz": z}, device_id_type=MESH)
    pl.semaphore_wait(barrier, 2)

    def send(way, n):
        l, first = place(1 - way, n)
        return pltpu.make_async_remote_copy(
            cc_v.at[gz, l, pl.ds(first, PIECE), :], late_o.at[way, n],
            (right_s, left_s)[way].at[n], (right_r, left_r)[way].at[n],
            device_id={"gx": gx, "gy": gy, "gz": (right, left)[way]}, device_id_type=MESH,
        )

    def skip(way, n):
        pass

    core = lax.rem(gy, 2)
    rest(core, skip, lambda way, n: send(way, n).start())
    rest(core, skip, lambda way, n: send(way, n).wait())


def write_kernel(nz, np_v, rn_v, cn_v, ap_v, cc_v, np_h, rn_h, cn_h, ap_h, cc_h, sem, part_sem):
    gy, gz = lax.axis_index("gy"), lax.axis_index("gz")
    right, left, across = lax.rem(gz + 1, nz), lax.rem(gz + nz - 1, nz), lax.rem(gz + 2, nz)
    copies = []

    def put(source, target):
        copies.append(pltpu.make_async_copy(source, target, sem.at[len(copies)]))
        copies[-1].start()

    def part(way, n):
        l, first = place(1 - way, n)
        rows = pl.ds(first, PIECE)
        owner = (left, right)[way]
        return pltpu.make_async_copy(
            cc_v.at[owner, l, rows, :], cc_h.at[l, rows, columns_of(owner)], part_sem.at[way * PIECES + n]
        )

    for l in range(LAYERS):
        put(np_v.at[l], np_h.at[l])
        put(ap_v.at[l], ap_h.at[l])
        for owner in (gz, across):
            put(cc_v.at[owner, l], cc_h.at[l, :, columns_of(owner)])
        for kind, owner in ((0, left), (1, right)):
            rows = pl.ds(2 * kind * PIECE, 2 * PIECE)
            put(cc_v.at[owner, l, rows, :], cc_h.at[l, rows, columns_of(owner)])
    put(rn_v, rn_h)
    put(cn_v, cn_h)

    def skip(way, n):
        pass

    core = lax.rem(gy, 2)
    rest(core, lambda way, n: part(way, n).start(), skip)
    for copy in copies:
        copy.wait()
    rest(core, lambda way, n: part(way, n).wait(), skip)


def finish_kernel(nz, late_v, old_h, cc_h, part_sem):
    gy, gz = lax.axis_index("gy"), lax.axis_index("gz")
    right, left = lax.rem(gz + 1, nz), lax.rem(gz + nz - 1, nz)

    def part(way, n):
        l, first = place(1 - way, n)
        rows = pl.ds(first, PIECE)
        return pltpu.make_async_copy(
            late_v.at[way, n], cc_h.at[l, rows, columns_of((left, right)[way])], part_sem.at[way * PIECES + n]
        )

    def skip(way, n):
        pass

    core = lax.rem(gy, 2)
    rest(core, skip, lambda way, n: part(way, n).start())
    rest(core, skip, lambda way, n: part(way, n).wait())


def solution(mesh):
    nx, ny, nz = (mesh.shape[a] for a in ("gx", "gy", "gz"))

    def body(params, grads, row_state, col_state):
        V = pltpu.VMEM
        sem = pltpu.SemaphoreType.DMA
        kept = pl.pallas_call(
            functools.partial(step_kernel, (nx, ny, nz)),
            out_shape=[
                V((LAYERS, ROWS, COLS), F32),
                V((LAYERS, ROWS), F32),
                V((LAYERS, COLS), F32),
                V((LAYERS, ROWS, COLS), F32),
                V((nz, LAYERS, ROWS, COLS), BF16),
            ],
            in_specs=[pl.BlockSpec(memory_space=pltpu.HBM)] * 4,
            out_specs=[pl.BlockSpec(memory_space=V)] * 5,
            scratch_shapes=[
                V((LAYERS, ROWS, COLS), BF16),
                V((LAYERS, ROWS), F32),
                V((LAYERS, COLS), F32),
                V((nz, LAYERS, 8, 128), F32),
                V((ny, LAYERS, 1, COLS), F32),
                V((nx * ny * nz, 1, 128), F32),
                V((LAYERS, 8, 128), F32),
                V((LAYERS, 1, COLS), F32),
                V((LAYERS, ROWS, 128), F32),
                sem((2 * LAYERS + 2,)),
                sem((nz - 1,)), sem((nz - 1,)),
                sem((ny - 1,)), sem((ny - 1,)),
                sem, sem,
                sem((3 * PIECES,)), sem((3 * PIECES,)),
                sem((3 * PIECES,)), sem((3 * PIECES,)),
            ],
            compiler_params=pltpu.CompilerParams(
                collective_id=0, has_side_effects=True, vmem_limit_bytes=16 * 2**20
            ),
        )(*[pltpu.with_memory_space_constraint(a, pltpu.HBM) for a in (params, grads, row_state, col_state)])
        new_params, row_new, col_new, applied, compute = pl.pallas_call(
            functools.partial(write_kernel, nz),
            out_shape=[
                jax.ShapeDtypeStruct((LAYERS, ROWS, COLS), F32),
                jax.ShapeDtypeStruct((LAYERS, ROWS), F32),
                jax.ShapeDtypeStruct((LAYERS, COLS), F32),
                jax.ShapeDtypeStruct((LAYERS, ROWS, COLS), F32),
                jax.ShapeDtypeStruct((LAYERS, ROWS, nz * COLS), BF16),
            ],
            in_specs=[pl.BlockSpec(memory_space=V)] * 5,
            out_specs=[pl.BlockSpec(memory_space=pltpu.HBM)] * 5,
            scratch_shapes=[sem((6 * LAYERS + 2,)), sem((2 * PIECES,))],
            compiler_params=pltpu.CompilerParams(vmem_limit_bytes=2**20),
        )(*kept)
        late = pl.pallas_call(
            functools.partial(rest_kernel, nz),
            out_shape=V((2, PIECES, PIECE, COLS), BF16),
            in_specs=[pl.BlockSpec(memory_space=V), pl.BlockSpec(memory_space=pltpu.HBM)],
            out_specs=pl.BlockSpec(memory_space=V),
            scratch_shapes=[sem((PIECES,)), sem((PIECES,)), sem((PIECES,)), sem((PIECES,))],
            compiler_params=pltpu.CompilerParams(collective_id=1, has_side_effects=True, vmem_limit_bytes=2**20),
        )(kept[4], pltpu.with_memory_space_constraint(col_new, pltpu.HBM))
        compute = pl.pallas_call(
            functools.partial(finish_kernel, nz),
            out_shape=jax.ShapeDtypeStruct((LAYERS, ROWS, nz * COLS), BF16),
            in_specs=[pl.BlockSpec(memory_space=V), pl.BlockSpec(memory_space=pltpu.HBM)],
            out_specs=pl.BlockSpec(memory_space=pltpu.HBM),
            scratch_shapes=[sem((2 * PIECES,))],
            input_output_aliases={1: 0},
            compiler_params=pltpu.CompilerParams(vmem_limit_bytes=2**20),
        )(late, compute)
        return new_params, row_new, col_new, applied, compute

    return jax.shard_map(
        body,
        mesh=mesh,
        in_specs=(P("gx", "gy", "gz"), P("gx", "gy", "gz"), P("gx", "gy"), P("gx", "gz")),
        out_specs=(
            P("gx", "gy", "gz"),
            P("gx", "gy"),
            P("gx", "gz"),
            P("gx", "gy", "gz"),
            P("gx", "gy", None),
        ),
        check_vma=False,
    )
```

```python
import functools

import jax
import jax.numpy as jnp
from jax import lax
from jax.experimental import pallas as pl
from jax.experimental.pallas import tpu as pltpu
from jax.sharding import PartitionSpec as P

MESH = pl.DeviceIdType.MESH
F32 = jnp.float32
BF16 = jnp.bfloat16

decay_rate = 0.842
tiny_term = 1e-30
step_share = 0.01
clip_limit = 1.0

LAYERS = 3
ROWS = 896
COLS = 384
STEP = 112
RAW = 64
PIECE = ROWS // 4
PIECES = 2 * LAYERS
EARLY = (0, 6)


def place(kind, n):
    first = (2 * kind + n % 2) * PIECE
    cut = RAW if n == 0 else 0
    return n // 2, first + cut, PIECE - cut


def lanes(shape):
    return lax.broadcasted_iota(jnp.int32, shape, len(shape) - 1)


def advance(weights, gradient, inv_col, factor):
    scaled = gradient.astype(F32) * inv_col
    step = jnp.concatenate([scaled[:, 128 * k : 128 * k + 128] * factor for k in range(COLS // 128)], axis=1)
    return step, weights - step_share * step


def total(x):
    return jnp.sum(jnp.sum(x, axis=0, keepdims=True), axis=1, keepdims=True)


def lane_of(x, k):
    return jnp.sum(jnp.where(lanes(x.shape) == k, x, 0.0), axis=1, keepdims=True)


def pack_rows(lane_dense):
    sub = lax.broadcasted_iota(jnp.int32, (8, 128), 0)
    lane = lanes((8, 128))
    source = lax.broadcasted_iota(jnp.int32, (128, 128), 0)
    target = lanes((128, 128))
    packed = None
    for k in range(ROWS // 128):
        pick = (target == source // 8 + 16 * k).astype(F32)
        spread = [
            jnp.where(lane % 8 == sub, jnp.broadcast_to(lane_dense[l : l + 1, 128 * k : 128 * (k + 1)], (8, 128)), 0.0)
            for l in range(LAYERS)
        ]
        part = jnp.dot(
            jnp.concatenate(spread, axis=0), pick, preferred_element_type=F32, precision=lax.Precision.HIGHEST
        )
        packed = part if packed is None else packed + part
    return packed


def unpack_rows(packed):
    sub = lax.broadcasted_iota(jnp.int32, (8, 128), 0)
    lane = lanes((8, 128))
    source = lax.broadcasted_iota(jnp.int32, (128, 128), 0)
    target = lanes((128, 128))
    out = []
    for k in range(ROWS // 128):
        pick = (source == target // 8 + 16 * k).astype(F32)
        part = jnp.dot(packed, pick, preferred_element_type=F32, precision=lax.Precision.HIGHEST)
        out.append(
            [
                jnp.sum(jnp.where(lane % 8 == sub, part[8 * l : 8 * (l + 1)], 0.0), axis=0, keepdims=True)
                for l in range(LAYERS)
            ]
        )
    return out


def step_kernel(
    sizes,
    p_h, g_h, rs_h, cs_h,
    np_o, rn_o, cn_o, ap_o, cc_o,
    g_v, rs_v, cs_v, raw_p, raw_g, inv_x, row_x, col_x, all_x, row_inv, col_inv, rrb,
    told_line, told_plane, load_sem, row_s, row_r, col_s, col_r, all_s, all_r,
    inv_s, inv_r, raw_right_s, raw_right_r, raw_left_s, raw_left_r,
    right_s, right_r, left_s, left_r,
):
    nx, ny, nz = sizes
    gx, gy, gz = lax.axis_index("gx"), lax.axis_index("gy"), lax.axis_index("gz")
    right, left = lax.rem(gz + 1, nz), lax.rem(gz + nz - 1, nz)
    columns = COLS * nz
    rows_all = ROWS * ny

    loads = [pltpu.make_async_copy(g_h.at[l], g_v.at[l], load_sem.at[l]) for l in range(LAYERS)]
    loads += [
        pltpu.make_async_copy(rs_h, rs_v, load_sem.at[LAYERS]),
        pltpu.make_async_copy(cs_h, cs_v, load_sem.at[LAYERS + 1]),
    ]
    loads += [pltpu.make_async_copy(p_h.at[l], np_o.at[l], load_sem.at[LAYERS + 2 + l]) for l in range(LAYERS)]
    for load in loads:
        load.start()

    xs = [lax.rem(gx + i, nx) for i in range(nx)]
    ys = [lax.rem(gy + i, ny) for i in range(ny)]
    zs = [lax.rem(gz + i, nz) for i in range(nz)]
    barrier = pltpu.get_barrier_semaphore()

    def signal(sem, peers):
        for i, j, k in peers:
            pl.semaphore_signal(sem, inc=1, device_id={"gx": xs[i], "gy": ys[j], "gz": zs[k]}, device_id_type=MESH)

    line_x = [(i, 0, 0) for i in range(1, nx)]
    line_y = [(0, j, 0) for j in range(1, ny)]
    line_z = [(0, 0, k) for k in range(1, nz)]
    signal(barrier, line_x + line_y + line_z)

    lane = lanes((8, 128))

    def stats(l, carry):
        pltpu.make_async_copy(g_h.at[l], g_v.at[l], load_sem.at[l]).wait()
        packed = jnp.zeros((8, 128), F32)
        col_acc = jnp.zeros((8, COLS), F32)
        for t in range(ROWS // 16):
            x = g_v[l, 16 * t : 16 * t + 16, :].astype(F32)
            sq = x * x
            row = jnp.sum(sq[:, 0:128] + sq[:, 128:256] + sq[:, 256:384], axis=1, keepdims=True)
            packed = jnp.where(lane == 2 * t, row[0:8], packed)
            packed = jnp.where(lane == 2 * t + 1, row[8:16], packed)
            col_acc = col_acc + sq[0:8] + sq[8:16]
        row_x[gz, l] = packed
        col_x[gy, l] = jnp.sum(col_acc, axis=0, keepdims=True)
        return carry

    lax.fori_loop(0, LAYERS, stats, 0)

    pl.semaphore_wait(barrier, len(line_x + line_y + line_z))
    for load in loads[LAYERS + 2 :]:
        load.wait()
    exchange = []
    for i in range(1, nz):
        exchange.append(
            pltpu.make_async_remote_copy(
                row_x.at[gz], row_x.at[gz], row_s.at[i - 1], row_r.at[i - 1],
                device_id={"gx": gx, "gy": gy, "gz": zs[i]}, device_id_type=MESH,
            )
        )
    for i in range(1, ny):
        exchange.append(
            pltpu.make_async_remote_copy(
                col_x.at[gy], col_x.at[gy], col_s.at[i - 1], col_r.at[i - 1],
                device_id={"gx": gx, "gy": ys[i], "gz": gz}, device_id_type=MESH,
            )
        )
    for copy in exchange:
        copy.start()
    signal(told_line, line_z)

    def raw(way, number):
        kind = way if number != 1 else 1 - way
        owner = (left, right)[way] if number == 2 else gz
        rows = pl.ds(2 * kind * PIECE, RAW)
        sources = (raw_p.at[owner, kind], raw_g.at[owner, kind]) if number == 2 else (np_o.at[0, rows], g_v.at[0, rows])
        return [
            pltpu.make_async_remote_copy(
                source, target.at[owner, kind],
                (raw_right_s, raw_left_s)[way].at[2 * number + k], (raw_right_r, raw_left_r)[way].at[2 * number + k],
                device_id={"gx": gx, "gy": gy, "gz": (right, left)[way]}, device_id_type=MESH,
            )
            for k, (source, target) in enumerate(zip(sources, (raw_p, raw_g)))
        ]

    raws = [[raw(way, number) for way in range(2)] for number in range(3)]
    for pair in raws[0]:
        for copy in pair:
            copy.start()

    row1 = lanes((1, 128))

    def weigh(l, payload):
        def some(i, acc):
            for t in range(STEP // 8):
                w = np_o[l, pl.ds(pl.multiple_of(i * STEP + 8 * t, 8), 8), :]
                acc = acc + w * w
            return acc

        squares = lax.fori_loop(0, ROWS // STEP, some, jnp.zeros((8, COLS), F32))
        return jnp.where(row1 == LAYERS + l, total(squares), payload)

    payload = lax.fori_loop(0, LAYERS, weigh, jnp.zeros((1, 128), F32))
    pl.semaphore_wait(told_line, len(line_z))
    signal(told_plane, line_y)
    loads[LAYERS].wait()
    loads[LAYERS + 1].wait()
    row_old = pack_rows(rs_v[...])

    for copy in exchange:
        copy.wait_recv()
    row_new = []
    for l in range(LAYERS):
        row_sum = row_x[0, l]
        for k in range(1, nz):
            row_sum = row_sum + row_x[k, l]
        new = decay_rate * row_old[8 * l : 8 * l + 8] + (1.0 - decay_rate) * (row_sum / columns + tiny_term)
        row_new.append(new)
        row_inv[l] = lax.rsqrt(new)
        payload = jnp.where(row1 == 2 * LAYERS + l, total(jnp.where(lane < ROWS // 8, new, 0.0)), payload)
        col_sum = col_x[0, l]
        for k in range(1, ny):
            col_sum = col_sum + col_x[k, l]
        new = decay_rate * cs_v[l : l + 1, :] + (1.0 - decay_rate) * (col_sum / rows_all + tiny_term)
        cn_o[l : l + 1, :] = new
        col_inv[l] = lax.rsqrt(new)
    inv_x[gz] = col_inv[0]
    inverse = [
        pltpu.make_async_remote_copy(
            inv_x.at[gz], inv_x.at[gz], inv_s.at[i - 1], inv_r.at[i - 1],
            device_id={"gx": gx, "gy": gy, "gz": zs[i]}, device_id_type=MESH,
        )
        for i in range(1, nz)
    ]
    for copy in inverse:
        copy.start()

    def updates(l, payload):
        acc = jnp.zeros((8, 128), F32)
        inv_packed = row_inv[l]
        inv_col = col_inv[l]
        for t in range(ROWS // 16):
            x = g_v[l, 16 * t : 16 * t + 16, :].astype(F32)
            u = x * inv_col
            sq = u * u
            y = sq[:, 0:128] + sq[:, 128:256] + sq[:, 256:384]
            for k in range(2):
                inv = jnp.sum(jnp.where(lane == 2 * t + k, inv_packed, 0.0), axis=1, keepdims=True)
                inv = jnp.broadcast_to(inv, (8, 128))
                rrb[l, 16 * t + 8 * k : 16 * t + 8 * k + 8, :] = inv
                acc = acc + y[8 * k : 8 * k + 8] * (inv * inv)
        return jnp.where(row1 == l, total(acc), payload)

    payload = lax.fori_loop(0, LAYERS, updates, payload)

    pl.semaphore_wait(told_plane, len(line_y))
    all_x[(gx * ny + gy) * nz + gz] = payload
    mine = all_x.at[(gx * ny + gy) * nz + gz]

    def far(at):
        return sum(min(a, n - a) for a, n in zip((at[0], at[1] // 2, at[2]), (nx, ny // 2, nz)))

    others = [(i, j, k) for i in range(nx) for j in range(ny) for k in range(nz) if i or j or k]
    for i, j, k in sorted(others, key=far, reverse=True):
        pltpu.make_async_remote_copy(
            mine, mine, all_s, all_r,
            device_id={"gx": xs[i], "gy": ys[j], "gz": zs[k]}, device_id_type=MESH,
        ).start()
    for pair in raws[1]:
        for copy in pair:
            copy.start()
    for way in range(2):
        for copy in raws[0][way]:
            copy.wait_recv()
        for copy in raws[2][way]:
            copy.start()
    pltpu.make_async_copy(all_x.at[pl.ds(0, len(others))], all_x.at[pl.ds(0, len(others))], all_r).wait()
    everything = jnp.zeros((1, 1), F32)
    scale = [jnp.zeros((1, 1), F32)] * LAYERS
    for i in range(nx):
        sums = jnp.sum(all_x[i * ny * nz : (i + 1) * ny * nz], axis=0)
        for l in range(LAYERS):
            mean_row = lane_of(sums, 2 * LAYERS + l) / (nz * rows_all)
            everything = everything + mean_row * lane_of(sums, l)
            root = jnp.sqrt(lane_of(sums, LAYERS + l) / (rows_all * columns)) * jnp.sqrt(mean_row)
            scale[l] = jnp.where(gx == i, root, scale[l])
    entries = float(nx * LAYERS * rows_all * columns)
    clip = jnp.maximum(1.0, jnp.sqrt(everything / entries) / clip_limit)
    scale = [one / clip for one in scale]

    def apply(l, first, size):
        inv_col = col_inv[l]

        tiles = size // 16
        at_once = max(k for k in range(1, 12) if tiles % k == 0)

        def some(i, carry):
            for t in range(at_once):
                rows = pl.ds(pl.multiple_of(first + (i * at_once + t) * 16, 16), 16)
                step, new = advance(np_o[l, rows, :], g_v[l, rows, :], inv_col, rrb[l, rows, :] * scale[l])
                ap_o[l, rows, :] = step
                np_o[l, rows, :] = new
                cc_o[gz, l, rows, :] = new.astype(BF16)
            return carry

        lax.fori_loop(0, tiles // at_once, some, 0)

    def apply_raw(owner):
        inv_col = inv_x[owner]
        for kind in range(2):
            for t in range(RAW // 16):
                rows = pl.ds(2 * kind * PIECE + 16 * t, 16)
                some = pl.ds(16 * t, 16)
                _, new = advance(
                    raw_p[owner, kind, some, :], raw_g[owner, kind, some, :], inv_col, rrb[0, rows, :] * scale[0]
                )
                cc_o[owner, 0, rows, :] = new.astype(BF16)

    def send(owner, kind, n, way, number):
        l, first, size = place(kind, n)
        piece = cc_o.at[owner, l, pl.ds(first, size), :]
        return pltpu.make_async_remote_copy(
            piece, piece, (right_s, left_s)[way].at[number], (right_r, left_r)[way].at[number],
            device_id={"gx": gx, "gy": gy, "gz": (right, left)[way]}, device_id_type=MESH,
        )

    core = lax.rem(gy, 2)
    own = ([send(gz, 0, n, 0, n) for n in range(PIECES)], [send(gz, 1, n, 1, n) for n in range(PIECES)])
    last = ([send(gz, 1, n, 0, PIECES + n) for n in range(PIECES)], [send(gz, 0, n, 1, PIECES + n) for n in range(PIECES)])
    on = (
        [send(left, 0, n, 0, 2 * PIECES + n) for n in range(PIECES)],
        [send(right, 1, n, 1, 2 * PIECES + n) for n in range(PIECES)],
    )
    for n in range(PIECES):
        for way in range(2):
            apply(*place(way, n))
            own[way][n].start()

    def extra(do):
        for n in range(min(EARLY)):
            for way in range(2):
                do(last[way][n])

        @pl.when(core == (0 if EARLY[0] > EARLY[1] else 1))
        def _():
            for n in range(min(EARLY), max(EARLY)):
                for way in range(2):
                    do(last[way][n])

    extra(lambda copy: copy.start())
    new_rows = unpack_rows(jnp.concatenate(row_new, axis=0))
    for k in range(ROWS // 128):
        for l in range(LAYERS):
            rn_o[l : l + 1, 128 * k : 128 * (k + 1)] = new_rows[k][l]

    for copy in inverse:
        copy.wait_recv()
    for number in (1, 2):
        for pair in raws[number]:
            for copy in pair:
                copy.wait_recv()
    for i in range(1, nz):
        apply_raw(zs[i])
    for number in range(3):
        for pair in raws[number]:
            for copy in pair:
                copy.wait_send()
    for kind in range(2):
        apply(0, 2 * kind * PIECE, RAW)
    for n in range(PIECES):
        for way in range(2):
            own[way][n].wait_recv()
            on[way][n].start()
    for way in range(2):
        for n in range(PIECES):
            on[way][n].wait_recv()
    extra(lambda copy: copy.wait_recv())
    for copy in exchange + inverse + own[0] + own[1] + on[0] + on[1]:
        copy.wait_send()
    extra(lambda copy: copy.wait_send())
    pltpu.make_async_copy(all_x.at[pl.ds(0, len(others))], all_x.at[pl.ds(0, len(others))], all_s).wait()


def rest(core, early, late):
    for n in range(PIECES):
        for way in range(2):
            if n < min(EARLY):
                early(way, n)
            elif n >= max(EARLY):
                late(way, n)

    ahead = 0 if EARLY[0] > EARLY[1] else 1
    for mine, do in ((ahead, early), (1 - ahead, late)):

        @pl.when(core == mine)
        def _(do=do):
            for n in range(min(EARLY), max(EARLY)):
                for way in range(2):
                    do(way, n)


def columns_of(owner):
    return pl.ds(pl.multiple_of(owner * COLS, COLS), COLS)


def rest_kernel(nz, cc_v, after_h, late_o, right_s, right_r, left_s, left_r):
    gx, gy, gz = lax.axis_index("gx"), lax.axis_index("gy"), lax.axis_index("gz")
    right, left = lax.rem(gz + 1, nz), lax.rem(gz + nz - 1, nz)
    barrier = pltpu.get_barrier_semaphore()
    for z in (right, left):
        pl.semaphore_signal(barrier, inc=1, device_id={"gx": gx, "gy": gy, "gz": z}, device_id_type=MESH)
    pl.semaphore_wait(barrier, 2)

    def send(way, n):
        l, first, size = place(1 - way, n)
        return pltpu.make_async_remote_copy(
            cc_v.at[gz, l, pl.ds(first, size), :], late_o.at[way, n, pl.ds(0, size), :],
            (right_s, left_s)[way].at[n], (right_r, left_r)[way].at[n],
            device_id={"gx": gx, "gy": gy, "gz": (right, left)[way]}, device_id_type=MESH,
        )

    def skip(way, n):
        pass

    core = lax.rem(gy, 2)
    rest(core, skip, lambda way, n: send(way, n).start())
    rest(core, skip, lambda way, n: send(way, n).wait())


def write_kernel(nz, np_v, rn_v, cn_v, ap_v, cc_v, np_h, rn_h, cn_h, ap_h, cc_h, sem, part_sem):
    gy, gz = lax.axis_index("gy"), lax.axis_index("gz")
    right, left, across = lax.rem(gz + 1, nz), lax.rem(gz + nz - 1, nz), lax.rem(gz + 2, nz)
    copies = []

    def put(source, target):
        copies.append(pltpu.make_async_copy(source, target, sem.at[len(copies)]))
        copies[-1].start()

    def part(way, n):
        l, first, size = place(1 - way, n)
        rows = pl.ds(first, size)
        owner = (left, right)[way]
        return pltpu.make_async_copy(
            cc_v.at[owner, l, rows, :], cc_h.at[l, rows, columns_of(owner)], part_sem.at[way * PIECES + n]
        )

    for l in range(LAYERS):
        put(np_v.at[l], np_h.at[l])
        put(ap_v.at[l], ap_h.at[l])
        for owner in (gz, across):
            put(cc_v.at[owner, l], cc_h.at[l, :, columns_of(owner)])
        for kind, owner in ((0, left), (1, right)):
            rows = pl.ds(2 * kind * PIECE, 2 * PIECE)
            put(cc_v.at[owner, l, rows, :], cc_h.at[l, rows, columns_of(owner)])
    for kind, owner in ((1, left), (0, right)):
        rows = pl.ds(2 * kind * PIECE, RAW)
        put(cc_v.at[owner, 0, rows, :], cc_h.at[0, rows, columns_of(owner)])
    put(rn_v, rn_h)
    put(cn_v, cn_h)

    def skip(way, n):
        pass

    core = lax.rem(gy, 2)
    rest(core, lambda way, n: part(way, n).start(), skip)
    for copy in copies:
        copy.wait()
    rest(core, lambda way, n: part(way, n).wait(), skip)


def finish_kernel(nz, late_v, old_h, cc_h, part_sem):
    gy, gz = lax.axis_index("gy"), lax.axis_index("gz")
    right, left = lax.rem(gz + 1, nz), lax.rem(gz + nz - 1, nz)

    def part(way, n):
        l, first, size = place(1 - way, n)
        rows = pl.ds(first, size)
        return pltpu.make_async_copy(
            late_v.at[way, n, pl.ds(0, size), :], cc_h.at[l, rows, columns_of((left, right)[way])], part_sem.at[way * PIECES + n]
        )

    def skip(way, n):
        pass

    core = lax.rem(gy, 2)
    rest(core, skip, lambda way, n: part(way, n).start())
    rest(core, skip, lambda way, n: part(way, n).wait())


def solution(mesh):
    nx, ny, nz = (mesh.shape[a] for a in ("gx", "gy", "gz"))

    def body(params, grads, row_state, col_state):
        V = pltpu.VMEM
        sem = pltpu.SemaphoreType.DMA
        kept = pl.pallas_call(
            functools.partial(step_kernel, (nx, ny, nz)),
            out_shape=[
                V((LAYERS, ROWS, COLS), F32),
                V((LAYERS, ROWS), F32),
                V((LAYERS, COLS), F32),
                V((LAYERS, ROWS, COLS), F32),
                V((nz, LAYERS, ROWS, COLS), BF16),
            ],
            in_specs=[pl.BlockSpec(memory_space=pltpu.HBM)] * 4,
            out_specs=[pl.BlockSpec(memory_space=V)] * 5,
            scratch_shapes=[
                V((LAYERS, ROWS, COLS), BF16),
                V((LAYERS, ROWS), F32),
                V((LAYERS, COLS), F32),
                V((nz, 2, RAW, COLS), F32),
                V((nz, 2, RAW, COLS), BF16),
                V((nz, 1, COLS), F32),
                V((nz, LAYERS, 8, 128), F32),
                V((ny, LAYERS, 1, COLS), F32),
                V((nx * ny * nz, 1, 128), F32),
                V((LAYERS, 8, 128), F32),
                V((LAYERS, 1, COLS), F32),
                V((LAYERS, ROWS, 128), F32),
                pltpu.SemaphoreType.REGULAR, pltpu.SemaphoreType.REGULAR,
                sem((2 * LAYERS + 2,)),
                sem((nz - 1,)), sem((nz - 1,)),
                sem((ny - 1,)), sem((ny - 1,)),
                sem, sem,
                sem((nz - 1,)), sem((nz - 1,)),
                sem((6,)), sem((6,)), sem((6,)), sem((6,)),
                sem((3 * PIECES,)), sem((3 * PIECES,)),
                sem((3 * PIECES,)), sem((3 * PIECES,)),
            ],
            compiler_params=pltpu.CompilerParams(
                collective_id=0, has_side_effects=True, vmem_limit_bytes=16 * 2**20
            ),
        )(*[pltpu.with_memory_space_constraint(a, pltpu.HBM) for a in (params, grads, row_state, col_state)])
        new_params, row_new, col_new, applied, compute = pl.pallas_call(
            functools.partial(write_kernel, nz),
            out_shape=[
                jax.ShapeDtypeStruct((LAYERS, ROWS, COLS), F32),
                jax.ShapeDtypeStruct((LAYERS, ROWS), F32),
                jax.ShapeDtypeStruct((LAYERS, COLS), F32),
                jax.ShapeDtypeStruct((LAYERS, ROWS, COLS), F32),
                jax.ShapeDtypeStruct((LAYERS, ROWS, nz * COLS), BF16),
            ],
            in_specs=[pl.BlockSpec(memory_space=V)] * 5,
            out_specs=[pl.BlockSpec(memory_space=pltpu.HBM)] * 5,
            scratch_shapes=[sem((6 * LAYERS + 4,)), sem((2 * PIECES,))],
            compiler_params=pltpu.CompilerParams(vmem_limit_bytes=2**20),
        )(*kept)
        late = pl.pallas_call(
            functools.partial(rest_kernel, nz),
            out_shape=V((2, PIECES, PIECE, COLS), BF16),
            in_specs=[pl.BlockSpec(memory_space=V), pl.BlockSpec(memory_space=pltpu.HBM)],
            out_specs=pl.BlockSpec(memory_space=V),
            scratch_shapes=[sem((PIECES,)), sem((PIECES,)), sem((PIECES,)), sem((PIECES,))],
            compiler_params=pltpu.CompilerParams(collective_id=1, has_side_effects=True, vmem_limit_bytes=2**20),
        )(kept[4], pltpu.with_memory_space_constraint(col_new, pltpu.HBM))
        compute = pl.pallas_call(
            functools.partial(finish_kernel, nz),
            out_shape=jax.ShapeDtypeStruct((LAYERS, ROWS, nz * COLS), BF16),
            in_specs=[pl.BlockSpec(memory_space=V), pl.BlockSpec(memory_space=pltpu.HBM)],
            out_specs=pl.BlockSpec(memory_space=pltpu.HBM),
            scratch_shapes=[sem((2 * PIECES,))],
            input_output_aliases={1: 0},
            compiler_params=pltpu.CompilerParams(vmem_limit_bytes=2**20),
        )(late, compute)
        return new_params, row_new, col_new, applied, compute

    return jax.shard_map(
        body,
        mesh=mesh,
        in_specs=(P("gx", "gy", "gz"), P("gx", "gy", "gz"), P("gx", "gy"), P("gx", "gz")),
        out_specs=(
            P("gx", "gy", "gz"),
            P("gx", "gy"),
            P("gx", "gz"),
            P("gx", "gy", "gz"),
            P("gx", "gy", None),
        ),
        check_vma=False,
    )
```

```python
import functools

import jax
import jax.numpy as jnp
from jax import lax
from jax.experimental import pallas as pl
from jax.experimental.pallas import tpu as pltpu
from jax.sharding import PartitionSpec as P

MESH = pl.DeviceIdType.MESH
F32 = jnp.float32
BF16 = jnp.bfloat16

decay_rate = 0.842
tiny_term = 1e-30
step_share = 0.01
clip_limit = 1.0

LAYERS = 3
ROWS = 896
COLS = 384
STEP = 112
RAW = 64
PIECE = ROWS // 4
PIECES = 2 * LAYERS
REST = 2
LATE_CORE = 0


def place(kind, n):
    first = (2 * kind + n % 2) * PIECE
    cut = RAW if n == 0 else 0
    return n // 2, first + cut, PIECE - cut


def stay(kind, n):
    cut = RAW if n == 0 else 0
    layers = pl.ds(0, 1) if n == 0 else pl.ds(1, LAYERS - 1)
    return layers, 2 * kind * PIECE + cut, 2 * PIECE - cut


def lanes(shape):
    return lax.broadcasted_iota(jnp.int32, shape, len(shape) - 1)


def advance(weights, gradient, inv_col, factor):
    scaled = gradient.astype(F32) * inv_col
    step = jnp.concatenate([scaled[:, 128 * k : 128 * k + 128] * factor for k in range(COLS // 128)], axis=1)
    return step, weights - step_share * step


def total(x):
    return jnp.sum(jnp.sum(x, axis=0, keepdims=True), axis=1, keepdims=True)


def lane_of(x, k):
    return jnp.sum(jnp.where(lanes(x.shape) == k, x, 0.0), axis=1, keepdims=True)


def pack_rows(lane_dense):
    sub = lax.broadcasted_iota(jnp.int32, (8, 128), 0)
    lane = lanes((8, 128))
    source = lax.broadcasted_iota(jnp.int32, (128, 128), 0)
    target = lanes((128, 128))
    packed = None
    for k in range(ROWS // 128):
        pick = (target == source // 8 + 16 * k).astype(F32)
        spread = [
            jnp.where(lane % 8 == sub, jnp.broadcast_to(lane_dense[l : l + 1, 128 * k : 128 * (k + 1)], (8, 128)), 0.0)
            for l in range(LAYERS)
        ]
        part = jnp.dot(
            jnp.concatenate(spread, axis=0), pick, preferred_element_type=F32, precision=lax.Precision.HIGHEST
        )
        packed = part if packed is None else packed + part
    return packed


def unpack_rows(packed):
    sub = lax.broadcasted_iota(jnp.int32, (8, 128), 0)
    lane = lanes((8, 128))
    source = lax.broadcasted_iota(jnp.int32, (128, 128), 0)
    target = lanes((128, 128))
    out = []
    for k in range(ROWS // 128):
        pick = (source == target // 8 + 16 * k).astype(F32)
        part = jnp.dot(packed, pick, preferred_element_type=F32, precision=lax.Precision.HIGHEST)
        out.append(
            [
                jnp.sum(jnp.where(lane % 8 == sub, part[8 * l : 8 * (l + 1)], 0.0), axis=0, keepdims=True)
                for l in range(LAYERS)
            ]
        )
    return out


def step_kernel(
    sizes,
    p_h, g_h, rs_h, cs_h,
    np_o, rn_o, cn_o, ap_o, cc_o,
    g_v, rs_v, cs_v, raw_p, raw_g, inv_x, row_x, col_x, all_x, row_inv, col_inv, col_w, rrb,
    told_line, told_plane, load_sem, row_s, row_r, col_s, col_r, all_s, all_r,
    inv_s, inv_r, raw_right_s, raw_right_r, raw_left_s, raw_left_r,
    right_s, right_r, left_s, left_r,
):
    nx, ny, nz = sizes
    gx, gy, gz = lax.axis_index("gx"), lax.axis_index("gy"), lax.axis_index("gz")
    right, left = lax.rem(gz + 1, nz), lax.rem(gz + nz - 1, nz)
    columns = COLS * nz
    rows_all = ROWS * ny

    loads = [pltpu.make_async_copy(g_h.at[l], g_v.at[l], load_sem.at[l]) for l in range(LAYERS)]
    loads += [
        pltpu.make_async_copy(rs_h, rs_v, load_sem.at[LAYERS]),
        pltpu.make_async_copy(cs_h, cs_v, load_sem.at[LAYERS + 1]),
    ]
    loads += [pltpu.make_async_copy(p_h.at[l], np_o.at[l], load_sem.at[LAYERS + 2 + l]) for l in range(LAYERS)]
    for load in loads:
        load.start()

    xs = [lax.rem(gx + i, nx) for i in range(nx)]
    ys = [lax.rem(gy + i, ny) for i in range(ny)]
    zs = [lax.rem(gz + i, nz) for i in range(nz)]
    barrier = pltpu.get_barrier_semaphore()

    def signal(sem, peers):
        for i, j, k in peers:
            pl.semaphore_signal(sem, inc=1, device_id={"gx": xs[i], "gy": ys[j], "gz": zs[k]}, device_id_type=MESH)

    line_x = [(i, 0, 0) for i in range(1, nx)]
    line_y = [(0, j, 0) for j in range(1, ny)]
    line_z = [(0, 0, k) for k in range(1, nz)]
    signal(barrier, line_x + line_y + line_z)

    lane = lanes((8, 128))

    def stats(l, carry):
        pltpu.make_async_copy(g_h.at[l], g_v.at[l], load_sem.at[l]).wait()
        packed = jnp.zeros((8, 128), F32)
        col_acc = jnp.zeros((8, COLS), F32)
        for t in range(ROWS // 16):
            x = g_v[l, 16 * t : 16 * t + 16, :].astype(F32)
            sq = x * x
            row = jnp.sum(sq[:, 0:128] + sq[:, 128:256] + sq[:, 256:384], axis=1, keepdims=True)
            packed = jnp.where(lane == 2 * t, row[0:8], packed)
            packed = jnp.where(lane == 2 * t + 1, row[8:16], packed)
            col_acc = col_acc + sq[0:8] + sq[8:16]
        row_x[gz, l] = packed
        col_x[gy, l] = jnp.sum(col_acc, axis=0, keepdims=True)
        return carry

    lax.fori_loop(0, LAYERS, stats, 0)

    pl.semaphore_wait(barrier, len(line_x + line_y + line_z))
    for load in loads[LAYERS + 2 :]:
        load.wait()
    exchange = []
    for i in range(1, nz):
        exchange.append(
            pltpu.make_async_remote_copy(
                row_x.at[gz], row_x.at[gz], row_s.at[i - 1], row_r.at[i - 1],
                device_id={"gx": gx, "gy": gy, "gz": zs[i]}, device_id_type=MESH,
            )
        )
    for i in range(1, ny):
        exchange.append(
            pltpu.make_async_remote_copy(
                col_x.at[gy], col_x.at[gy], col_s.at[i - 1], col_r.at[i - 1],
                device_id={"gx": gx, "gy": ys[i], "gz": gz}, device_id_type=MESH,
            )
        )
    for copy in exchange:
        copy.start()
    signal(told_line, line_z)

    def raw(way, number):
        kind = way if number != 1 else 1 - way
        owner = (left, right)[way] if number == 2 else gz
        rows = pl.ds(2 * kind * PIECE, RAW)
        sources = (raw_p.at[owner, kind], raw_g.at[owner, kind]) if number == 2 else (np_o.at[0, rows], g_v.at[0, rows])
        return [
            pltpu.make_async_remote_copy(
                source, target.at[owner, kind],
                (raw_right_s, raw_left_s)[way].at[2 * number + k], (raw_right_r, raw_left_r)[way].at[2 * number + k],
                device_id={"gx": gx, "gy": gy, "gz": (right, left)[way]}, device_id_type=MESH,
            )
            for k, (source, target) in enumerate(zip(sources, (raw_p, raw_g)))
        ]

    raws = [[raw(way, number) for way in range(2)] for number in range(3)]
    for pair in raws[0]:
        for copy in pair:
            copy.start()

    row1 = lanes((1, 128))

    def weigh(l, payload):
        def some(i, acc):
            for t in range(STEP // 8):
                w = np_o[l, pl.ds(pl.multiple_of(i * STEP + 8 * t, 8), 8), :]
                acc = acc + w * w
            for t in range(STEP // 16):
                rows = pl.ds(pl.multiple_of(i * STEP + 16 * t, 16), 16)
                x = g_v[l, rows, :].astype(F32)
                ap_o[l, rows, :] = x * x
            return acc

        squares = lax.fori_loop(0, ROWS // STEP, some, jnp.zeros((8, COLS), F32))
        return jnp.where(row1 == LAYERS + l, total(squares), payload)

    payload = lax.fori_loop(0, LAYERS, weigh, jnp.zeros((1, 128), F32))
    pl.semaphore_wait(told_line, len(line_z))
    signal(told_plane, line_y)
    loads[LAYERS].wait()
    loads[LAYERS + 1].wait()
    row_old = pack_rows(rs_v[...])

    for copy in exchange[: nz - 1]:
        copy.wait_recv()
    row_new = []
    for l in range(LAYERS):
        row_sum = row_x[0, l]
        for k in range(1, nz):
            row_sum = row_sum + row_x[k, l]
        new = decay_rate * row_old[8 * l : 8 * l + 8] + (1.0 - decay_rate) * (row_sum / columns + tiny_term)
        row_new.append(new)
        row_inv[l] = lax.rsqrt(new)
        payload = jnp.where(row1 == 2 * LAYERS + l, total(jnp.where(lane < ROWS // 8, new, 0.0)), payload)

    def updates(l, carry):
        acc = [jnp.zeros((8, 128), F32)] * (COLS // 128)
        inv_packed = row_inv[l]
        for t in range(ROWS // 8):
            inv = jnp.sum(jnp.where(lane == t, inv_packed, 0.0), axis=1, keepdims=True)
            inv = jnp.broadcast_to(inv, (8, 128))
            rrb[l, 8 * t : 8 * t + 8, :] = inv
            inv = inv * inv
            for k in range(COLS // 128):
                acc[k] = acc[k] + ap_o[l, 8 * t : 8 * t + 8, 128 * k : 128 * k + 128] * inv
        col_w[l] = jnp.sum(jnp.concatenate(acc, axis=1), axis=0, keepdims=True)
        return carry

    lax.fori_loop(0, LAYERS, updates, 0)
    for copy in exchange[nz - 1 :]:
        copy.wait_recv()
    for l in range(LAYERS):
        col_sum = col_x[0, l]
        for k in range(1, ny):
            col_sum = col_sum + col_x[k, l]
        new = decay_rate * cs_v[l : l + 1, :] + (1.0 - decay_rate) * (col_sum / rows_all + tiny_term)
        cn_o[l : l + 1, :] = new
        inv = lax.rsqrt(new)
        col_inv[l] = inv
        payload = jnp.where(row1 == l, total(col_w[l] * (inv * inv)), payload)
    inv_x[gz] = col_inv[0]
    inverse = [
        pltpu.make_async_remote_copy(
            inv_x.at[gz], inv_x.at[gz], inv_s.at[i - 1], inv_r.at[i - 1],
            device_id={"gx": gx, "gy": gy, "gz": zs[i]}, device_id_type=MESH,
        )
        for i in range(1, nz)
    ]

    pl.semaphore_wait(told_plane, len(line_y))
    all_x[(gx * ny + gy) * nz + gz] = payload
    mine = all_x.at[(gx * ny + gy) * nz + gz]

    def far(at):
        return sum(min(a, n - a) for a, n in zip((at[0], at[1] // 2, at[2]), (nx, ny // 2, nz)))

    others = [(i, j, k) for i in range(nx) for j in range(ny) for k in range(nz) if i or j or k]
    for i, j, k in sorted(others, key=far, reverse=True):
        pltpu.make_async_remote_copy(
            mine, mine, all_s, all_r,
            device_id={"gx": xs[i], "gy": ys[j], "gz": zs[k]}, device_id_type=MESH,
        ).start()
    for copy in inverse:
        copy.start()
    for pair in raws[1]:
        for copy in pair:
            copy.start()
    for way in range(2):
        for copy in raws[0][way]:
            copy.wait_recv()
        for copy in raws[2][way]:
            copy.start()
    pltpu.make_async_copy(all_x.at[pl.ds(0, len(others))], all_x.at[pl.ds(0, len(others))], all_r).wait()
    everything = jnp.zeros((1, 1), F32)
    scale = [jnp.zeros((1, 1), F32)] * LAYERS
    for i in range(nx):
        sums = jnp.sum(all_x[i * ny * nz : (i + 1) * ny * nz], axis=0)
        for l in range(LAYERS):
            mean_row = lane_of(sums, 2 * LAYERS + l) / (nz * rows_all)
            everything = everything + mean_row * lane_of(sums, l)
            root = jnp.sqrt(lane_of(sums, LAYERS + l) / (rows_all * columns)) * jnp.sqrt(mean_row)
            scale[l] = jnp.where(gx == i, root, scale[l])
    entries = float(nx * LAYERS * rows_all * columns)
    clip = jnp.maximum(1.0, jnp.sqrt(everything / entries) / clip_limit)
    scale = [one / clip for one in scale]

    def apply(l, first, size):
        inv_col = col_inv[l]

        tiles = size // 16
        at_once = max(k for k in range(1, 12) if tiles % k == 0)

        def some(i, carry):
            for t in range(at_once):
                rows = pl.ds(pl.multiple_of(first + (i * at_once + t) * 16, 16), 16)
                step, new = advance(np_o[l, rows, :], g_v[l, rows, :], inv_col, rrb[l, rows, :] * scale[l])
                ap_o[l, rows, :] = step
                np_o[l, rows, :] = new
                cc_o[gz, l, rows, :] = new.astype(BF16)
            return carry

        lax.fori_loop(0, tiles // at_once, some, 0)

    def apply_raw(owner):
        inv_col = inv_x[owner]
        for kind in range(2):
            for t in range(RAW // 16):
                rows = pl.ds(2 * kind * PIECE + 16 * t, 16)
                some = pl.ds(16 * t, 16)
                _, new = advance(
                    raw_p[owner, kind, some, :], raw_g[owner, kind, some, :], inv_col, rrb[0, rows, :] * scale[0]
                )
                cc_o[owner, 0, rows, :] = new.astype(BF16)

    def send(owner, kind, n, way, number):
        l, first, size = place(kind, n)
        piece = cc_o.at[owner, l, pl.ds(first, size), :]
        return pltpu.make_async_remote_copy(
            piece, piece, (right_s, left_s)[way].at[number], (right_r, left_r)[way].at[number],
            device_id={"gx": gx, "gy": gy, "gz": (right, left)[way]}, device_id_type=MESH,
        )

    core = lax.rem(gy, 2)
    own = ([send(gz, 0, n, 0, n) for n in range(PIECES)], [send(gz, 1, n, 1, n) for n in range(PIECES)])
    last = []
    for way in range(2):
        for n in range(REST):
            layers, first, size = stay(1 - way, n)
            piece = cc_o.at[gz, layers, pl.ds(first, size), :]
            last.append(
                pltpu.make_async_remote_copy(
                    piece, piece, (right_s, left_s)[way].at[2 * PIECES + n], (right_r, left_r)[way].at[2 * PIECES + n],
                    device_id={"gx": gx, "gy": gy, "gz": (right, left)[way]}, device_id_type=MESH,
                )
            )
    on = (
        [send(left, 0, n, 0, PIECES + n) for n in range(PIECES)],
        [send(right, 1, n, 1, PIECES + n) for n in range(PIECES)],
    )
    for n in range(PIECES):
        for way in range(2):
            apply(*place(way, n))
            own[way][n].start()

    new_rows = unpack_rows(jnp.concatenate(row_new, axis=0))
    for k in range(ROWS // 128):
        for l in range(LAYERS):
            rn_o[l : l + 1, 128 * k : 128 * (k + 1)] = new_rows[k][l]

    for copy in inverse:
        copy.wait_recv()
    for number in (1, 2):
        for pair in raws[number]:
            for copy in pair:
                copy.wait_recv()
    for i in range(1, nz):
        apply_raw(zs[i])
    for number in range(3):
        for pair in raws[number]:
            for copy in pair:
                copy.wait_send()
    for kind in range(2):
        apply(0, 2 * kind * PIECE, RAW)
    for n in range(PIECES):
        for way in range(2):
            own[way][n].wait_recv()
            on[way][n].start()

    @pl.when(core != LATE_CORE)
    def _():
        for copy in last:
            copy.start()

    for way in range(2):
        for n in range(PIECES):
            on[way][n].wait_recv()

    @pl.when(core != LATE_CORE)
    def _():
        for copy in last:
            copy.wait()

    for copy in exchange + inverse + own[0] + own[1] + on[0] + on[1]:
        copy.wait_send()
    pltpu.make_async_copy(all_x.at[pl.ds(0, len(others))], all_x.at[pl.ds(0, len(others))], all_s).wait()


def each(do):
    for way in range(2):
        for n in range(REST):
            do(way, n)


def columns_of(owner):
    return pl.ds(pl.multiple_of(owner * COLS, COLS), COLS)


def rest_kernel(nz, cc_v, after_h, late_o, right_s, right_r, left_s, left_r):
    gx, gy, gz = lax.axis_index("gx"), lax.axis_index("gy"), lax.axis_index("gz")
    right, left = lax.rem(gz + 1, nz), lax.rem(gz + nz - 1, nz)
    barrier = pltpu.get_barrier_semaphore()
    for z in (right, left):
        pl.semaphore_signal(barrier, inc=1, device_id={"gx": gx, "gy": gy, "gz": z}, device_id_type=MESH)
    pl.semaphore_wait(barrier, 2)

    def send(way, n):
        layers, first, size = stay(1 - way, n)
        return pltpu.make_async_remote_copy(
            cc_v.at[gz, layers, pl.ds(first, size), :], late_o.at[way, layers, pl.ds(2 * PIECE - size, size), :],
            (right_s, left_s)[way].at[n], (right_r, left_r)[way].at[n],
            device_id={"gx": gx, "gy": gy, "gz": (right, left)[way]}, device_id_type=MESH,
        )

    @pl.when(lax.rem(gy, 2) == LATE_CORE)
    def _():
        each(lambda way, n: send(way, n).start())
        each(lambda way, n: send(way, n).wait())


def write_kernel(nz, np_v, rn_v, cn_v, ap_v, cc_v, np_h, rn_h, cn_h, ap_h, cc_h, sem, part_sem):
    gy, gz = lax.axis_index("gy"), lax.axis_index("gz")
    right, left, across = lax.rem(gz + 1, nz), lax.rem(gz + nz - 1, nz), lax.rem(gz + 2, nz)
    copies = []

    def put(source, target):
        copies.append(pltpu.make_async_copy(source, target, sem.at[len(copies)]))
        copies[-1].start()

    def part(way, n):
        layers, first, size = stay(1 - way, n)
        rows = pl.ds(first, size)
        owner = (left, right)[way]
        return pltpu.make_async_copy(
            cc_v.at[owner, layers, rows, :], cc_h.at[layers, rows, columns_of(owner)], part_sem.at[way * REST + n]
        )

    early = lax.rem(gy, 2) != LATE_CORE

    @pl.when(early)
    def _():
        each(lambda way, n: part(way, n).start())

    for l in range(LAYERS):
        put(np_v.at[l], np_h.at[l])
        put(ap_v.at[l], ap_h.at[l])
        for owner in (gz, across):
            put(cc_v.at[owner, l], cc_h.at[l, :, columns_of(owner)])
        for kind, owner in ((0, left), (1, right)):
            rows = pl.ds(2 * kind * PIECE, 2 * PIECE)
            put(cc_v.at[owner, l, rows, :], cc_h.at[l, rows, columns_of(owner)])
    for kind, owner in ((1, left), (0, right)):
        rows = pl.ds(2 * kind * PIECE, RAW)
        put(cc_v.at[owner, 0, rows, :], cc_h.at[0, rows, columns_of(owner)])
    put(rn_v, rn_h)
    put(cn_v, cn_h)

    for copy in copies:
        copy.wait()

    @pl.when(early)
    def _():
        each(lambda way, n: part(way, n).wait())


def finish_kernel(nz, late_v, old_h, cc_h, part_sem):
    gy, gz = lax.axis_index("gy"), lax.axis_index("gz")
    right, left = lax.rem(gz + 1, nz), lax.rem(gz + nz - 1, nz)

    def part(way, n):
        layers, first, size = stay(1 - way, n)
        return pltpu.make_async_copy(
            late_v.at[way, layers, pl.ds(2 * PIECE - size, size), :],
            cc_h.at[layers, pl.ds(first, size), columns_of((left, right)[way])], part_sem.at[way * REST + n],
        )

    @pl.when(lax.rem(gy, 2) == LATE_CORE)
    def _():
        each(lambda way, n: part(way, n).start())
        each(lambda way, n: part(way, n).wait())


def solution(mesh):
    nx, ny, nz = (mesh.shape[a] for a in ("gx", "gy", "gz"))

    def body(params, grads, row_state, col_state):
        V = pltpu.VMEM
        sem = pltpu.SemaphoreType.DMA
        kept = pl.pallas_call(
            functools.partial(step_kernel, (nx, ny, nz)),
            out_shape=[
                V((LAYERS, ROWS, COLS), F32),
                V((LAYERS, ROWS), F32),
                V((LAYERS, COLS), F32),
                V((LAYERS, ROWS, COLS), F32),
                V((nz, LAYERS, ROWS, COLS), BF16),
            ],
            in_specs=[pl.BlockSpec(memory_space=pltpu.HBM)] * 4,
            out_specs=[pl.BlockSpec(memory_space=V)] * 5,
            scratch_shapes=[
                V((LAYERS, ROWS, COLS), BF16),
                V((LAYERS, ROWS), F32),
                V((LAYERS, COLS), F32),
                V((nz, 2, RAW, COLS), F32),
                V((nz, 2, RAW, COLS), BF16),
                V((nz, 1, COLS), F32),
                V((nz, LAYERS, 8, 128), F32),
                V((ny, LAYERS, 1, COLS), F32),
                V((nx * ny * nz, 1, 128), F32),
                V((LAYERS, 8, 128), F32),
                V((LAYERS, 1, COLS), F32),
                V((LAYERS, 1, COLS), F32),
                V((LAYERS, ROWS, 128), F32),
                pltpu.SemaphoreType.REGULAR, pltpu.SemaphoreType.REGULAR,
                sem((2 * LAYERS + 2,)),
                sem((nz - 1,)), sem((nz - 1,)),
                sem((ny - 1,)), sem((ny - 1,)),
                sem, sem,
                sem((nz - 1,)), sem((nz - 1,)),
                sem((6,)), sem((6,)), sem((6,)), sem((6,)),
                sem((2 * PIECES + REST,)), sem((2 * PIECES + REST,)),
                sem((2 * PIECES + REST,)), sem((2 * PIECES + REST,)),
            ],
            compiler_params=pltpu.CompilerParams(
                collective_id=0, has_side_effects=True, vmem_limit_bytes=16 * 2**20
            ),
        )(*[pltpu.with_memory_space_constraint(a, pltpu.HBM) for a in (params, grads, row_state, col_state)])
        new_params, row_new, col_new, applied, compute = pl.pallas_call(
            functools.partial(write_kernel, nz),
            out_shape=[
                jax.ShapeDtypeStruct((LAYERS, ROWS, COLS), F32),
                jax.ShapeDtypeStruct((LAYERS, ROWS), F32),
                jax.ShapeDtypeStruct((LAYERS, COLS), F32),
                jax.ShapeDtypeStruct((LAYERS, ROWS, COLS), F32),
                jax.ShapeDtypeStruct((LAYERS, ROWS, nz * COLS), BF16),
            ],
            in_specs=[pl.BlockSpec(memory_space=V)] * 5,
            out_specs=[pl.BlockSpec(memory_space=pltpu.HBM)] * 5,
            scratch_shapes=[sem((6 * LAYERS + 4,)), sem((2 * REST,))],
            compiler_params=pltpu.CompilerParams(vmem_limit_bytes=2**20),
        )(*kept)
        late = pl.pallas_call(
            functools.partial(rest_kernel, nz),
            out_shape=V((2, LAYERS, 2 * PIECE, COLS), BF16),
            in_specs=[pl.BlockSpec(memory_space=V), pl.BlockSpec(memory_space=pltpu.HBM)],
            out_specs=pl.BlockSpec(memory_space=V),
            scratch_shapes=[sem((REST,)), sem((REST,)), sem((REST,)), sem((REST,))],
            compiler_params=pltpu.CompilerParams(collective_id=1, has_side_effects=True, vmem_limit_bytes=2**20),
        )(kept[4], pltpu.with_memory_space_constraint(col_new, pltpu.HBM))
        compute = pl.pallas_call(
            functools.partial(finish_kernel, nz),
            out_shape=jax.ShapeDtypeStruct((LAYERS, ROWS, nz * COLS), BF16),
            in_specs=[pl.BlockSpec(memory_space=V), pl.BlockSpec(memory_space=pltpu.HBM)],
            out_specs=pl.BlockSpec(memory_space=pltpu.HBM),
            scratch_shapes=[sem((2 * REST,))],
            input_output_aliases={1: 0},
            compiler_params=pltpu.CompilerParams(vmem_limit_bytes=2**20),
        )(late, compute)
        return new_params, row_new, col_new, applied, compute

    return jax.shard_map(
        body,
        mesh=mesh,
        in_specs=(P("gx", "gy", "gz"), P("gx", "gy", "gz"), P("gx", "gy"), P("gx", "gz")),
        out_specs=(
            P("gx", "gy", "gz"),
            P("gx", "gy"),
            P("gx", "gz"),
            P("gx", "gy", "gz"),
            P("gx", "gy", None),
        ),
        check_vma=False,
    )
```

```python
import functools

import jax
import jax.numpy as jnp
from jax import lax
from jax.experimental import pallas as pl
from jax.experimental.pallas import tpu as pltpu
from jax.sharding import PartitionSpec as P

MESH = pl.DeviceIdType.MESH
F32 = jnp.float32
BF16 = jnp.bfloat16

decay_rate = 0.842
tiny_term = 1e-30
step_share = 0.01
clip_limit = 1.0

LAYERS = 3
ROWS = 896
COLS = 384
STEP = 112
RAW = 64
PIECE = ROWS // 4
PIECES = 2 * LAYERS
REST = 2
LATE_CORE = 1


def place(kind, n):
    first = (2 * kind + n % 2) * PIECE
    cut = RAW if n == 0 else 0
    return n // 2, first + cut, PIECE - cut


def stay(kind, n):
    cut = RAW if n == 0 else 0
    layers = pl.ds(0, 1) if n == 0 else pl.ds(1, LAYERS - 1)
    return layers, 2 * kind * PIECE + cut, 2 * PIECE - cut


def lanes(shape):
    return lax.broadcasted_iota(jnp.int32, shape, len(shape) - 1)


def advance(weights, gradient, inv_col, factor):
    scaled = gradient.astype(F32) * inv_col
    step = jnp.concatenate([scaled[:, 128 * k : 128 * k + 128] * factor for k in range(COLS // 128)], axis=1)
    return step, weights - step_share * step


def total(x):
    return jnp.sum(jnp.sum(x, axis=0, keepdims=True), axis=1, keepdims=True)


def lane_of(x, k):
    return jnp.sum(jnp.where(lanes(x.shape) == k, x, 0.0), axis=1, keepdims=True)


def pack_rows(lane_dense):
    sub = lax.broadcasted_iota(jnp.int32, (8, 128), 0)
    lane = lanes((8, 128))
    source = lax.broadcasted_iota(jnp.int32, (128, 128), 0)
    target = lanes((128, 128))
    packed = None
    for k in range(ROWS // 128):
        pick = (target == source // 8 + 16 * k).astype(F32)
        spread = [
            jnp.where(lane % 8 == sub, jnp.broadcast_to(lane_dense[l : l + 1, 128 * k : 128 * (k + 1)], (8, 128)), 0.0)
            for l in range(LAYERS)
        ]
        part = jnp.dot(
            jnp.concatenate(spread, axis=0), pick, preferred_element_type=F32, precision=lax.Precision.HIGHEST
        )
        packed = part if packed is None else packed + part
    return packed


def unpack_rows(packed):
    sub = lax.broadcasted_iota(jnp.int32, (8, 128), 0)
    lane = lanes((8, 128))
    source = lax.broadcasted_iota(jnp.int32, (128, 128), 0)
    target = lanes((128, 128))
    out = []
    for k in range(ROWS // 128):
        pick = (source == target // 8 + 16 * k).astype(F32)
        part = jnp.dot(packed, pick, preferred_element_type=F32, precision=lax.Precision.HIGHEST)
        out.append(
            [
                jnp.sum(jnp.where(lane % 8 == sub, part[8 * l : 8 * (l + 1)], 0.0), axis=0, keepdims=True)
                for l in range(LAYERS)
            ]
        )
    return out


def step_kernel(
    sizes,
    p_h, g_h, rs_h, cs_h,
    np_o, rn_o, cn_o, ap_o, cc_o,
    g_v, rs_v, cs_v, raw_p, raw_g, inv_x, row_x, col_x, all_x, row_inv, col_inv, col_w, rrb,
    told_line, told_plane, load_sem, row_s, row_r, col_s, col_r, all_s, all_r,
    inv_s, inv_r, raw_right_s, raw_right_r, raw_left_s, raw_left_r,
    right_s, right_r, left_s, left_r,
):
    nx, ny, nz = sizes
    gx, gy, gz = lax.axis_index("gx"), lax.axis_index("gy"), lax.axis_index("gz")
    right, left = lax.rem(gz + 1, nz), lax.rem(gz + nz - 1, nz)
    columns = COLS * nz
    rows_all = ROWS * ny

    loads = [pltpu.make_async_copy(g_h.at[l], g_v.at[l], load_sem.at[l]) for l in range(LAYERS)]
    loads += [
        pltpu.make_async_copy(rs_h, rs_v, load_sem.at[LAYERS]),
        pltpu.make_async_copy(cs_h, cs_v, load_sem.at[LAYERS + 1]),
    ]
    loads += [pltpu.make_async_copy(p_h.at[l], np_o.at[l], load_sem.at[LAYERS + 2 + l]) for l in range(LAYERS)]
    for load in loads:
        load.start()

    xs = [lax.rem(gx + i, nx) for i in range(nx)]
    ys = [lax.rem(gy + i, ny) for i in range(ny)]
    zs = [lax.rem(gz + i, nz) for i in range(nz)]
    barrier = pltpu.get_barrier_semaphore()

    def signal(sem, peers):
        for i, j, k in peers:
            pl.semaphore_signal(sem, inc=1, device_id={"gx": xs[i], "gy": ys[j], "gz": zs[k]}, device_id_type=MESH)

    line_x = [(i, 0, 0) for i in range(1, nx)]
    line_y = [(0, j, 0) for j in range(1, ny)]
    line_z = [(0, 0, k) for k in range(1, nz)]
    signal(barrier, line_x + line_y + line_z)

    lane = lanes((8, 128))

    def stats(l, carry):
        pltpu.make_async_copy(g_h.at[l], g_v.at[l], load_sem.at[l]).wait()
        packed = jnp.zeros((8, 128), F32)
        col_acc = jnp.zeros((8, COLS), F32)
        for t in range(ROWS // 16):
            x = g_v[l, 16 * t : 16 * t + 16, :].astype(F32)
            sq = x * x
            row = jnp.sum(sq[:, 0:128] + sq[:, 128:256] + sq[:, 256:384], axis=1, keepdims=True)
            packed = jnp.where(lane == 2 * t, row[0:8], packed)
            packed = jnp.where(lane == 2 * t + 1, row[8:16], packed)
            col_acc = col_acc + sq[0:8] + sq[8:16]
        row_x[gz, l] = packed
        col_x[gy, l] = jnp.sum(col_acc, axis=0, keepdims=True)
        return carry

    lax.fori_loop(0, LAYERS, stats, 0)

    pl.semaphore_wait(barrier, len(line_x + line_y + line_z))
    for load in loads[LAYERS + 2 :]:
        load.wait()
    exchange = []
    for i in range(1, nz):
        exchange.append(
            pltpu.make_async_remote_copy(
                row_x.at[gz], row_x.at[gz], row_s.at[i - 1], row_r.at[i - 1],
                device_id={"gx": gx, "gy": gy, "gz": zs[i]}, device_id_type=MESH,
            )
        )
    for i in range(1, ny):
        exchange.append(
            pltpu.make_async_remote_copy(
                col_x.at[gy], col_x.at[gy], col_s.at[i - 1], col_r.at[i - 1],
                device_id={"gx": gx, "gy": ys[i], "gz": gz}, device_id_type=MESH,
            )
        )
    for copy in exchange:
        copy.start()
    signal(told_line, line_z)

    def raw(way, number):
        kind = way if number != 1 else 1 - way
        owner = (left, right)[way] if number == 2 else gz
        rows = pl.ds(2 * kind * PIECE, RAW)
        sources = (raw_p.at[owner, kind], raw_g.at[owner, kind]) if number == 2 else (np_o.at[0, rows], g_v.at[0, rows])
        return [
            pltpu.make_async_remote_copy(
                source, target.at[owner, kind],
                (raw_right_s, raw_left_s)[way].at[2 * number + k], (raw_right_r, raw_left_r)[way].at[2 * number + k],
                device_id={"gx": gx, "gy": gy, "gz": (right, left)[way]}, device_id_type=MESH,
            )
            for k, (source, target) in enumerate(zip(sources, (raw_p, raw_g)))
        ]

    raws = [[raw(way, number) for way in range(2)] for number in range(3)]
    for pair in raws[0]:
        for copy in pair:
            copy.start()

    row1 = lanes((1, 128))

    def weigh(l, payload):
        def some(i, acc):
            for t in range(STEP // 8):
                w = np_o[l, pl.ds(pl.multiple_of(i * STEP + 8 * t, 8), 8), :]
                acc = acc + w * w
            for t in range(STEP // 16):
                rows = pl.ds(pl.multiple_of(i * STEP + 16 * t, 16), 16)
                x = g_v[l, rows, :].astype(F32)
                ap_o[l, rows, :] = x * x
            return acc

        squares = lax.fori_loop(0, ROWS // STEP, some, jnp.zeros((8, COLS), F32))
        return jnp.where(row1 == LAYERS + l, total(squares), payload)

    payload = lax.fori_loop(0, LAYERS, weigh, jnp.zeros((1, 128), F32))
    pl.semaphore_wait(told_line, len(line_z))
    signal(told_plane, line_y)
    loads[LAYERS].wait()
    loads[LAYERS + 1].wait()
    row_old = pack_rows(rs_v[...])

    for copy in exchange[: nz - 1]:
        copy.wait_recv()
    row_new = []
    for l in range(LAYERS):
        row_sum = row_x[0, l]
        for k in range(1, nz):
            row_sum = row_sum + row_x[k, l]
        new = decay_rate * row_old[8 * l : 8 * l + 8] + (1.0 - decay_rate) * (row_sum / columns + tiny_term)
        row_new.append(new)
        row_inv[l] = lax.rsqrt(new)
        payload = jnp.where(row1 == 2 * LAYERS + l, total(jnp.where(lane < ROWS // 8, new, 0.0)), payload)

    def updates(l, carry):
        acc = [jnp.zeros((8, 128), F32)] * (COLS // 128)
        inv_packed = row_inv[l]
        for t in range(ROWS // 8):
            inv = jnp.sum(jnp.where(lane == t, inv_packed, 0.0), axis=1, keepdims=True)
            inv = jnp.broadcast_to(inv, (8, 128))
            rrb[l, 8 * t : 8 * t + 8, :] = inv
            inv = inv * inv
            for k in range(COLS // 128):
                acc[k] = acc[k] + ap_o[l, 8 * t : 8 * t + 8, 128 * k : 128 * k + 128] * inv
        col_w[l] = jnp.sum(jnp.concatenate(acc, axis=1), axis=0, keepdims=True)
        return carry

    lax.fori_loop(0, LAYERS, updates, 0)
    for copy in exchange[nz - 1 :]:
        copy.wait_recv()
    for l in range(LAYERS):
        col_sum = col_x[0, l]
        for k in range(1, ny):
            col_sum = col_sum + col_x[k, l]
        new = decay_rate * cs_v[l : l + 1, :] + (1.0 - decay_rate) * (col_sum / rows_all + tiny_term)
        cn_o[l : l + 1, :] = new
        inv = lax.rsqrt(new)
        col_inv[l] = inv
        payload = jnp.where(row1 == l, total(col_w[l] * (inv * inv)), payload)
    inv_x[gz] = col_inv[0]
    inverse = [
        pltpu.make_async_remote_copy(
            inv_x.at[gz], inv_x.at[gz], inv_s.at[i - 1], inv_r.at[i - 1],
            device_id={"gx": gx, "gy": gy, "gz": zs[i]}, device_id_type=MESH,
        )
        for i in range(1, nz)
    ]

    pl.semaphore_wait(told_plane, len(line_y))
    all_x[(gx * ny + gy) * nz + gz] = payload
    mine = all_x.at[(gx * ny + gy) * nz + gz]

    def far(at):
        return sum(min(a, n - a) for a, n in zip((at[0], at[1] // 2, at[2]), (nx, ny // 2, nz)))

    others = [(i, j, k) for i in range(nx) for j in range(ny) for k in range(nz) if i or j or k]
    for i, j, k in sorted(others, key=far, reverse=True):
        pltpu.make_async_remote_copy(
            mine, mine, all_s, all_r,
            device_id={"gx": xs[i], "gy": ys[j], "gz": zs[k]}, device_id_type=MESH,
        ).start()
    for copy in inverse:
        copy.start()
    for pair in raws[1]:
        for copy in pair:
            copy.start()
    for way in range(2):
        for copy in raws[0][way]:
            copy.wait_recv()
        for copy in raws[2][way]:
            copy.start()
    pltpu.make_async_copy(all_x.at[pl.ds(0, len(others))], all_x.at[pl.ds(0, len(others))], all_r).wait()
    everything = jnp.zeros((1, 1), F32)
    scale = [jnp.zeros((1, 1), F32)] * LAYERS
    for i in range(nx):
        sums = jnp.sum(all_x[i * ny * nz : (i + 1) * ny * nz], axis=0)
        for l in range(LAYERS):
            mean_row = lane_of(sums, 2 * LAYERS + l) / (nz * rows_all)
            everything = everything + mean_row * lane_of(sums, l)
            root = jnp.sqrt(lane_of(sums, LAYERS + l) / (rows_all * columns)) * jnp.sqrt(mean_row)
            scale[l] = jnp.where(gx == i, root, scale[l])
    entries = float(nx * LAYERS * rows_all * columns)
    clip = jnp.maximum(1.0, jnp.sqrt(everything / entries) / clip_limit)
    scale = [one / clip for one in scale]

    def apply(l, first, size):
        inv_col = col_inv[l]

        tiles = size // 16
        at_once = max(k for k in range(1, 12) if tiles % k == 0)

        def some(i, carry):
            for t in range(at_once):
                rows = pl.ds(pl.multiple_of(first + (i * at_once + t) * 16, 16), 16)
                step, new = advance(np_o[l, rows, :], g_v[l, rows, :], inv_col, rrb[l, rows, :] * scale[l])
                ap_o[l, rows, :] = step
                np_o[l, rows, :] = new
                cc_o[gz, l, rows, :] = new.astype(BF16)
            return carry

        lax.fori_loop(0, tiles // at_once, some, 0)

    def apply_raw(owner):
        inv_col = inv_x[owner]
        for kind in range(2):
            for t in range(RAW // 16):
                rows = pl.ds(2 * kind * PIECE + 16 * t, 16)
                some = pl.ds(16 * t, 16)
                _, new = advance(
                    raw_p[owner, kind, some, :], raw_g[owner, kind, some, :], inv_col, rrb[0, rows, :] * scale[0]
                )
                cc_o[owner, 0, rows, :] = new.astype(BF16)

    def send(owner, kind, n, way, number):
        l, first, size = place(kind, n)
        piece = cc_o.at[owner, l, pl.ds(first, size), :]
        return pltpu.make_async_remote_copy(
            piece, piece, (right_s, left_s)[way].at[number], (right_r, left_r)[way].at[number],
            device_id={"gx": gx, "gy": gy, "gz": (right, left)[way]}, device_id_type=MESH,
        )

    core = lax.rem(gy, 2)
    own = ([send(gz, 0, n, 0, n) for n in range(PIECES)], [send(gz, 1, n, 1, n) for n in range(PIECES)])
    last = []
    for way in range(2):
        for n in range(REST):
            layers, first, size = stay(1 - way, n)
            piece = cc_o.at[gz, layers, pl.ds(first, size), :]
            last.append(
                pltpu.make_async_remote_copy(
                    piece, piece, (right_s, left_s)[way].at[2 * PIECES + n], (right_r, left_r)[way].at[2 * PIECES + n],
                    device_id={"gx": gx, "gy": gy, "gz": (right, left)[way]}, device_id_type=MESH,
                )
            )
    on = (
        [send(left, 0, n, 0, PIECES + n) for n in range(PIECES)],
        [send(right, 1, n, 1, PIECES + n) for n in range(PIECES)],
    )
    for n in range(PIECES):
        for way in range(2):
            apply(*place(way, n))
            own[way][n].start()

    new_rows = unpack_rows(jnp.concatenate(row_new, axis=0))
    for k in range(ROWS // 128):
        for l in range(LAYERS):
            rn_o[l : l + 1, 128 * k : 128 * (k + 1)] = new_rows[k][l]

    for copy in inverse:
        copy.wait_recv()
    for number in (1, 2):
        for pair in raws[number]:
            for copy in pair:
                copy.wait_recv()
    for i in range(1, nz):
        apply_raw(zs[i])
    for number in range(3):
        for pair in raws[number]:
            for copy in pair:
                copy.wait_send()
    for kind in range(2):
        apply(0, 2 * kind * PIECE, RAW)
    for n in range(PIECES):
        for way in range(2):
            own[way][n].wait_recv()
            on[way][n].start()

    @pl.when(core != LATE_CORE)
    def _():
        for copy in last:
            copy.start()

    for way in range(2):
        for n in range(PIECES):
            on[way][n].wait_recv()

    @pl.when(core != LATE_CORE)
    def _():
        for copy in last:
            copy.wait()

    for copy in exchange + inverse + own[0] + own[1] + on[0] + on[1]:
        copy.wait_send()
    pltpu.make_async_copy(all_x.at[pl.ds(0, len(others))], all_x.at[pl.ds(0, len(others))], all_s).wait()


def each(do):
    for way in range(2):
        for n in range(REST):
            do(way, n)


def columns_of(owner):
    return pl.ds(pl.multiple_of(owner * COLS, COLS), COLS)


def rest_kernel(nz, cc_v, after_h, late_o, right_s, right_r, left_s, left_r):
    gx, gy, gz = lax.axis_index("gx"), lax.axis_index("gy"), lax.axis_index("gz")
    right, left = lax.rem(gz + 1, nz), lax.rem(gz + nz - 1, nz)
    barrier = pltpu.get_barrier_semaphore()
    for z in (right, left):
        pl.semaphore_signal(barrier, inc=1, device_id={"gx": gx, "gy": gy, "gz": z}, device_id_type=MESH)
    pl.semaphore_wait(barrier, 2)

    def send(way, n):
        layers, first, size = stay(1 - way, n)
        return pltpu.make_async_remote_copy(
            cc_v.at[gz, layers, pl.ds(first, size), :], late_o.at[way, layers, pl.ds(2 * PIECE - size, size), :],
            (right_s, left_s)[way].at[n], (right_r, left_r)[way].at[n],
            device_id={"gx": gx, "gy": gy, "gz": (right, left)[way]}, device_id_type=MESH,
        )

    @pl.when(lax.rem(gy, 2) == LATE_CORE)
    def _():
        each(lambda way, n: send(way, n).start())
        each(lambda way, n: send(way, n).wait())


def write_kernel(nz, np_v, rn_v, cn_v, ap_v, cc_v, np_h, rn_h, cn_h, ap_h, cc_h, sem, part_sem):
    gy, gz = lax.axis_index("gy"), lax.axis_index("gz")
    right, left, across = lax.rem(gz + 1, nz), lax.rem(gz + nz - 1, nz), lax.rem(gz + 2, nz)
    copies = []

    def put(source, target):
        copies.append(pltpu.make_async_copy(source, target, sem.at[len(copies)]))
        copies[-1].start()

    def part(way, n):
        layers, first, size = stay(1 - way, n)
        rows = pl.ds(first, size)
        owner = (left, right)[way]
        return pltpu.make_async_copy(
            cc_v.at[owner, layers, rows, :], cc_h.at[layers, rows, columns_of(owner)], part_sem.at[way * REST + n]
        )

    early = lax.rem(gy, 2) != LATE_CORE

    @pl.when(early)
    def _():
        each(lambda way, n: part(way, n).start())

    for l in range(LAYERS):
        put(np_v.at[l], np_h.at[l])
        put(ap_v.at[l], ap_h.at[l])
        for owner in (gz, across):
            put(cc_v.at[owner, l], cc_h.at[l, :, columns_of(owner)])
        for kind, owner in ((0, left), (1, right)):
            rows = pl.ds(2 * kind * PIECE, 2 * PIECE)
            put(cc_v.at[owner, l, rows, :], cc_h.at[l, rows, columns_of(owner)])
    for kind, owner in ((1, left), (0, right)):
        rows = pl.ds(2 * kind * PIECE, RAW)
        put(cc_v.at[owner, 0, rows, :], cc_h.at[0, rows, columns_of(owner)])
    put(rn_v, rn_h)
    put(cn_v, cn_h)

    for copy in copies:
        copy.wait()

    @pl.when(early)
    def _():
        each(lambda way, n: part(way, n).wait())


def finish_kernel(nz, late_v, old_h, cc_h, part_sem):
    gy, gz = lax.axis_index("gy"), lax.axis_index("gz")
    right, left = lax.rem(gz + 1, nz), lax.rem(gz + nz - 1, nz)

    def part(way, n):
        layers, first, size = stay(1 - way, n)
        return pltpu.make_async_copy(
            late_v.at[way, layers, pl.ds(2 * PIECE - size, size), :],
            cc_h.at[layers, pl.ds(first, size), columns_of((left, right)[way])], part_sem.at[way * REST + n],
        )

    @pl.when(lax.rem(gy, 2) == LATE_CORE)
    def _():
        each(lambda way, n: part(way, n).start())
        each(lambda way, n: part(way, n).wait())


def solution(mesh):
    nx, ny, nz = (mesh.shape[a] for a in ("gx", "gy", "gz"))

    def body(params, grads, row_state, col_state):
        V = pltpu.VMEM
        sem = pltpu.SemaphoreType.DMA
        kept = pl.pallas_call(
            functools.partial(step_kernel, (nx, ny, nz)),
            out_shape=[
                V((LAYERS, ROWS, COLS), F32),
                V((LAYERS, ROWS), F32),
                V((LAYERS, COLS), F32),
                V((LAYERS, ROWS, COLS), F32),
                V((nz, LAYERS, ROWS, COLS), BF16),
            ],
            in_specs=[pl.BlockSpec(memory_space=pltpu.HBM)] * 4,
            out_specs=[pl.BlockSpec(memory_space=V)] * 5,
            scratch_shapes=[
                V((LAYERS, ROWS, COLS), BF16),
                V((LAYERS, ROWS), F32),
                V((LAYERS, COLS), F32),
                V((nz, 2, RAW, COLS), F32),
                V((nz, 2, RAW, COLS), BF16),
                V((nz, 1, COLS), F32),
                V((nz, LAYERS, 8, 128), F32),
                V((ny, LAYERS, 1, COLS), F32),
                V((nx * ny * nz, 1, 128), F32),
                V((LAYERS, 8, 128), F32),
                V((LAYERS, 1, COLS), F32),
                V((LAYERS, 1, COLS), F32),
                V((LAYERS, ROWS, 128), F32),
                pltpu.SemaphoreType.REGULAR, pltpu.SemaphoreType.REGULAR,
                sem((2 * LAYERS + 2,)),
                sem((nz - 1,)), sem((nz - 1,)),
                sem((ny - 1,)), sem((ny - 1,)),
                sem, sem,
                sem((nz - 1,)), sem((nz - 1,)),
                sem((6,)), sem((6,)), sem((6,)), sem((6,)),
                sem((2 * PIECES + REST,)), sem((2 * PIECES + REST,)),
                sem((2 * PIECES + REST,)), sem((2 * PIECES + REST,)),
            ],
            compiler_params=pltpu.CompilerParams(
                collective_id=0, has_side_effects=True, vmem_limit_bytes=16 * 2**20
            ),
        )(*[pltpu.with_memory_space_constraint(a, pltpu.HBM) for a in (params, grads, row_state, col_state)])
        new_params, row_new, col_new, applied, compute = pl.pallas_call(
            functools.partial(write_kernel, nz),
            out_shape=[
                jax.ShapeDtypeStruct((LAYERS, ROWS, COLS), F32),
                jax.ShapeDtypeStruct((LAYERS, ROWS), F32),
                jax.ShapeDtypeStruct((LAYERS, COLS), F32),
                jax.ShapeDtypeStruct((LAYERS, ROWS, COLS), F32),
                jax.ShapeDtypeStruct((LAYERS, ROWS, nz * COLS), BF16),
            ],
            in_specs=[pl.BlockSpec(memory_space=V)] * 5,
            out_specs=[pl.BlockSpec(memory_space=pltpu.HBM)] * 5,
            scratch_shapes=[sem((6 * LAYERS + 4,)), sem((2 * REST,))],
            compiler_params=pltpu.CompilerParams(vmem_limit_bytes=2**20),
        )(*kept)
        late = pl.pallas_call(
            functools.partial(rest_kernel, nz),
            out_shape=V((2, LAYERS, 2 * PIECE, COLS), BF16),
            in_specs=[pl.BlockSpec(memory_space=V), pl.BlockSpec(memory_space=pltpu.HBM)],
            out_specs=pl.BlockSpec(memory_space=V),
            scratch_shapes=[sem((REST,)), sem((REST,)), sem((REST,)), sem((REST,))],
            compiler_params=pltpu.CompilerParams(collective_id=1, has_side_effects=True, vmem_limit_bytes=2**20),
        )(kept[4], pltpu.with_memory_space_constraint(col_new, pltpu.HBM))
        compute = pl.pallas_call(
            functools.partial(finish_kernel, nz),
            out_shape=jax.ShapeDtypeStruct((LAYERS, ROWS, nz * COLS), BF16),
            in_specs=[pl.BlockSpec(memory_space=V), pl.BlockSpec(memory_space=pltpu.HBM)],
            out_specs=pl.BlockSpec(memory_space=pltpu.HBM),
            scratch_shapes=[sem((2 * REST,))],
            input_output_aliases={1: 0},
            compiler_params=pltpu.CompilerParams(vmem_limit_bytes=2**20),
        )(late, compute)
        return new_params, row_new, col_new, applied, compute

    return jax.shard_map(
        body,
        mesh=mesh,
        in_specs=(P("gx", "gy", "gz"), P("gx", "gy", "gz"), P("gx", "gy"), P("gx", "gz")),
        out_specs=(
            P("gx", "gy", "gz"),
            P("gx", "gy"),
            P("gx", "gz"),
            P("gx", "gy", "gz"),
            P("gx", "gy", None),
        ),
        check_vma=False,
    )
```

```python
import functools

import jax
import jax.numpy as jnp
from jax import lax
from jax.experimental import pallas as pl
from jax.experimental.pallas import tpu as pltpu
from jax.sharding import PartitionSpec as P

MESH = pl.DeviceIdType.MESH
F32 = jnp.float32
BF16 = jnp.bfloat16

decay_rate = 0.842
tiny_term = 1e-30
step_share = 0.01
clip_limit = 1.0

LAYERS = 3
ROWS = 896
COLS = 384
STEP = 112
RAW = 80
PIECE = ROWS // 4
PIECES = 2 * LAYERS
REST = 2
LATE_CORE = 1


def place(kind, n):
    first = (2 * kind + n % 2) * PIECE
    cut = RAW if n == 0 else 0
    return n // 2, first + cut, PIECE - cut


def stay(kind, n):
    cut = RAW if n == 0 else 0
    layers = pl.ds(0, 1) if n == 0 else pl.ds(1, LAYERS - 1)
    return layers, 2 * kind * PIECE + cut, 2 * PIECE - cut


def lanes(shape):
    return lax.broadcasted_iota(jnp.int32, shape, len(shape) - 1)


def advance(weights, gradient, inv_col, factor):
    scaled = gradient.astype(F32) * inv_col
    step = jnp.concatenate([scaled[:, 128 * k : 128 * k + 128] * factor for k in range(COLS // 128)], axis=1)
    return step, weights - step_share * step


def total(x):
    return jnp.sum(jnp.sum(x, axis=0, keepdims=True), axis=1, keepdims=True)


def lane_of(x, k):
    return jnp.sum(jnp.where(lanes(x.shape) == k, x, 0.0), axis=1, keepdims=True)


def pack_rows(lane_dense):
    sub = lax.broadcasted_iota(jnp.int32, (8, 128), 0)
    lane = lanes((8, 128))
    source = lax.broadcasted_iota(jnp.int32, (128, 128), 0)
    target = lanes((128, 128))
    packed = None
    for k in range(ROWS // 128):
        pick = (target == source // 8 + 16 * k).astype(F32)
        spread = [
            jnp.where(lane % 8 == sub, jnp.broadcast_to(lane_dense[l : l + 1, 128 * k : 128 * (k + 1)], (8, 128)), 0.0)
            for l in range(LAYERS)
        ]
        part = jnp.dot(
            jnp.concatenate(spread, axis=0), pick, preferred_element_type=F32, precision=lax.Precision.HIGHEST
        )
        packed = part if packed is None else packed + part
    return packed


def unpack_rows(packed):
    sub = lax.broadcasted_iota(jnp.int32, (8, 128), 0)
    lane = lanes((8, 128))
    source = lax.broadcasted_iota(jnp.int32, (128, 128), 0)
    target = lanes((128, 128))
    out = []
    for k in range(ROWS // 128):
        pick = (source == target // 8 + 16 * k).astype(F32)
        part = jnp.dot(packed, pick, preferred_element_type=F32, precision=lax.Precision.HIGHEST)
        out.append(
            [
                jnp.sum(jnp.where(lane % 8 == sub, part[8 * l : 8 * (l + 1)], 0.0), axis=0, keepdims=True)
                for l in range(LAYERS)
            ]
        )
    return out


def step_kernel(
    sizes,
    p_h, g_h, rs_h, cs_h,
    np_o, rn_o, cn_o, ap_o, cc_o,
    g_v, rs_v, cs_v, raw_p, raw_g, inv_x, row_x, col_x, all_x, row_inv, col_inv, col_w, rrb,
    told_line, told_plane, load_sem, row_s, row_r, col_s, col_r, all_s, all_r,
    inv_s, inv_r, raw_right_s, raw_right_r, raw_left_s, raw_left_r,
    right_s, right_r, left_s, left_r,
):
    nx, ny, nz = sizes
    gx, gy, gz = lax.axis_index("gx"), lax.axis_index("gy"), lax.axis_index("gz")
    right, left = lax.rem(gz + 1, nz), lax.rem(gz + nz - 1, nz)
    columns = COLS * nz
    rows_all = ROWS * ny

    loads = [pltpu.make_async_copy(g_h.at[l], g_v.at[l], load_sem.at[l]) for l in range(LAYERS)]
    loads += [
        pltpu.make_async_copy(rs_h, rs_v, load_sem.at[LAYERS]),
        pltpu.make_async_copy(cs_h, cs_v, load_sem.at[LAYERS + 1]),
    ]
    loads += [pltpu.make_async_copy(p_h.at[l], np_o.at[l], load_sem.at[LAYERS + 2 + l]) for l in range(LAYERS)]
    for load in loads:
        load.start()

    xs = [lax.rem(gx + i, nx) for i in range(nx)]
    ys = [lax.rem(gy + i, ny) for i in range(ny)]
    zs = [lax.rem(gz + i, nz) for i in range(nz)]
    barrier = pltpu.get_barrier_semaphore()

    def signal(sem, peers):
        for i, j, k in peers:
            pl.semaphore_signal(sem, inc=1, device_id={"gx": xs[i], "gy": ys[j], "gz": zs[k]}, device_id_type=MESH)

    line_x = [(i, 0, 0) for i in range(1, nx)]
    line_y = [(0, j, 0) for j in range(1, ny)]
    line_z = [(0, 0, k) for k in range(1, nz)]
    signal(barrier, line_x + line_y + line_z)

    lane = lanes((8, 128))

    def stats(l, carry):
        pltpu.make_async_copy(g_h.at[l], g_v.at[l], load_sem.at[l]).wait()
        packed = jnp.zeros((8, 128), F32)
        col_acc = jnp.zeros((8, COLS), F32)
        for t in range(ROWS // 16):
            x = g_v[l, 16 * t : 16 * t + 16, :].astype(F32)
            sq = x * x
            row = jnp.sum(sq[:, 0:128] + sq[:, 128:256] + sq[:, 256:384], axis=1, keepdims=True)
            packed = jnp.where(lane == 2 * t, row[0:8], packed)
            packed = jnp.where(lane == 2 * t + 1, row[8:16], packed)
            col_acc = col_acc + sq[0:8] + sq[8:16]
        row_x[gz, l] = packed
        col_x[gy, l] = jnp.sum(col_acc, axis=0, keepdims=True)
        return carry

    lax.fori_loop(0, LAYERS, stats, 0)

    pl.semaphore_wait(barrier, len(line_x + line_y + line_z))
    for load in loads[LAYERS + 2 :]:
        load.wait()
    exchange = []
    for i in range(1, nz):
        exchange.append(
            pltpu.make_async_remote_copy(
                row_x.at[gz], row_x.at[gz], row_s.at[i - 1], row_r.at[i - 1],
                device_id={"gx": gx, "gy": gy, "gz": zs[i]}, device_id_type=MESH,
            )
        )
    for i in range(1, ny):
        exchange.append(
            pltpu.make_async_remote_copy(
                col_x.at[gy], col_x.at[gy], col_s.at[i - 1], col_r.at[i - 1],
                device_id={"gx": gx, "gy": ys[i], "gz": gz}, device_id_type=MESH,
            )
        )
    for copy in exchange:
        copy.start()
    signal(told_line, line_z)

    def raw(way, number):
        kind = way if number != 1 else 1 - way
        owner = (left, right)[way] if number == 2 else gz
        rows = pl.ds(2 * kind * PIECE, RAW)
        sources = (raw_p.at[owner, kind], raw_g.at[owner, kind]) if number == 2 else (np_o.at[0, rows], g_v.at[0, rows])
        return [
            pltpu.make_async_remote_copy(
                source, target.at[owner, kind],
                (raw_right_s, raw_left_s)[way].at[2 * number + k], (raw_right_r, raw_left_r)[way].at[2 * number + k],
                device_id={"gx": gx, "gy": gy, "gz": (right, left)[way]}, device_id_type=MESH,
            )
            for k, (source, target) in enumerate(zip(sources, (raw_p, raw_g)))
        ]

    raws = [[raw(way, number) for way in range(2)] for number in range(3)]
    for pair in raws[0]:
        for copy in pair:
            copy.start()
    near = jnp.logical_and(gx == 0, gy // 2 == 0)

    @pl.when(near)
    def _():
        for pair in raws[1]:
            for copy in pair:
                copy.start()


    row1 = lanes((1, 128))

    def weigh(l, payload):
        def some(i, acc):
            for t in range(STEP // 8):
                w = np_o[l, pl.ds(pl.multiple_of(i * STEP + 8 * t, 8), 8), :]
                acc = acc + w * w
            for t in range(STEP // 16):
                rows = pl.ds(pl.multiple_of(i * STEP + 16 * t, 16), 16)
                x = g_v[l, rows, :].astype(F32)
                ap_o[l, rows, :] = x * x
            return acc

        squares = lax.fori_loop(0, ROWS // STEP, some, jnp.zeros((8, COLS), F32))
        return jnp.where(row1 == LAYERS + l, total(squares), payload)

    payload = lax.fori_loop(0, LAYERS, weigh, jnp.zeros((1, 128), F32))
    pl.semaphore_wait(told_line, len(line_z))
    signal(told_plane, line_y)
    loads[LAYERS].wait()
    loads[LAYERS + 1].wait()
    row_old = pack_rows(rs_v[...])

    for copy in exchange[: nz - 1]:
        copy.wait_recv()
    row_new = []
    for l in range(LAYERS):
        row_sum = row_x[0, l]
        for k in range(1, nz):
            row_sum = row_sum + row_x[k, l]
        new = decay_rate * row_old[8 * l : 8 * l + 8] + (1.0 - decay_rate) * (row_sum / columns + tiny_term)
        row_new.append(new)
        row_inv[l] = lax.rsqrt(new)
        payload = jnp.where(row1 == 2 * LAYERS + l, total(jnp.where(lane < ROWS // 8, new, 0.0)), payload)

    def updates(l, carry):
        acc = [jnp.zeros((8, 128), F32)] * (COLS // 128)
        inv_packed = row_inv[l]
        for t in range(ROWS // 8):
            inv = jnp.sum(jnp.where(lane == t, inv_packed, 0.0), axis=1, keepdims=True)
            inv = jnp.broadcast_to(inv, (8, 128))
            rrb[l, 8 * t : 8 * t + 8, :] = inv
            inv = inv * inv
            for k in range(COLS // 128):
                acc[k] = acc[k] + ap_o[l, 8 * t : 8 * t + 8, 128 * k : 128 * k + 128] * inv
        col_w[l] = jnp.sum(jnp.concatenate(acc, axis=1), axis=0, keepdims=True)
        return carry

    lax.fori_loop(0, LAYERS, updates, 0)
    for copy in exchange[nz - 1 :]:
        copy.wait_recv()
    for l in range(LAYERS):
        col_sum = col_x[0, l]
        for k in range(1, ny):
            col_sum = col_sum + col_x[k, l]
        new = decay_rate * cs_v[l : l + 1, :] + (1.0 - decay_rate) * (col_sum / rows_all + tiny_term)
        cn_o[l : l + 1, :] = new
        inv = lax.rsqrt(new)
        col_inv[l] = inv
        payload = jnp.where(row1 == l, total(col_w[l] * (inv * inv)), payload)
    inv_x[gz] = col_inv[0]
    inverse = [
        pltpu.make_async_remote_copy(
            inv_x.at[gz], inv_x.at[gz], inv_s.at[i - 1], inv_r.at[i - 1],
            device_id={"gx": gx, "gy": gy, "gz": zs[i]}, device_id_type=MESH,
        )
        for i in range(1, nz)
    ]

    pl.semaphore_wait(told_plane, len(line_y))
    all_x[(gx * ny + gy) * nz + gz] = payload
    mine = all_x.at[(gx * ny + gy) * nz + gz]

    def far(at):
        return sum(min(a, n - a) for a, n in zip((at[0], at[1] // 2, at[2]), (nx, ny // 2, nz)))

    others = [(i, j, k) for i in range(nx) for j in range(ny) for k in range(nz) if i or j or k]
    for i, j, k in sorted(others, key=far, reverse=True):
        pltpu.make_async_remote_copy(
            mine, mine, all_s, all_r,
            device_id={"gx": xs[i], "gy": ys[j], "gz": zs[k]}, device_id_type=MESH,
        ).start()
    for copy in inverse:
        copy.start()
    @pl.when(jnp.logical_not(near))
    def _():
        for pair in raws[1]:
            for copy in pair:
                copy.start()

    for way in range(2):
        for copy in raws[0][way]:
            copy.wait_recv()
        for copy in raws[2][way]:
            copy.start()
    pltpu.make_async_copy(all_x.at[pl.ds(0, len(others))], all_x.at[pl.ds(0, len(others))], all_r).wait()
    everything = jnp.zeros((1, 1), F32)
    scale = [jnp.zeros((1, 1), F32)] * LAYERS
    for i in range(nx):
        sums = jnp.sum(all_x[i * ny * nz : (i + 1) * ny * nz], axis=0)
        for l in range(LAYERS):
            mean_row = lane_of(sums, 2 * LAYERS + l) / (nz * rows_all)
            everything = everything + mean_row * lane_of(sums, l)
            root = jnp.sqrt(lane_of(sums, LAYERS + l) / (rows_all * columns)) * jnp.sqrt(mean_row)
            scale[l] = jnp.where(gx == i, root, scale[l])
    entries = float(nx * LAYERS * rows_all * columns)
    clip = jnp.maximum(1.0, jnp.sqrt(everything / entries) / clip_limit)
    scale = [one / clip for one in scale]

    def apply(l, first, size):
        inv_col = col_inv[l]

        tiles = size // 16
        at_once = max(k for k in range(1, 12) if tiles % k == 0)

        def some(i, carry):
            for t in range(at_once):
                rows = pl.ds(pl.multiple_of(first + (i * at_once + t) * 16, 16), 16)
                step, new = advance(np_o[l, rows, :], g_v[l, rows, :], inv_col, rrb[l, rows, :] * scale[l])
                ap_o[l, rows, :] = step
                np_o[l, rows, :] = new
                cc_o[gz, l, rows, :] = new.astype(BF16)
            return carry

        lax.fori_loop(0, tiles // at_once, some, 0)

    def apply_raw(owner):
        inv_col = inv_x[owner]
        for kind in range(2):
            for t in range(RAW // 16):
                rows = pl.ds(2 * kind * PIECE + 16 * t, 16)
                some = pl.ds(16 * t, 16)
                _, new = advance(
                    raw_p[owner, kind, some, :], raw_g[owner, kind, some, :], inv_col, rrb[0, rows, :] * scale[0]
                )
                cc_o[owner, 0, rows, :] = new.astype(BF16)

    def send(owner, kind, n, way, number):
        l, first, size = place(kind, n)
        piece = cc_o.at[owner, l, pl.ds(first, size), :]
        return pltpu.make_async_remote_copy(
            piece, piece, (right_s, left_s)[way].at[number], (right_r, left_r)[way].at[number],
            device_id={"gx": gx, "gy": gy, "gz": (right, left)[way]}, device_id_type=MESH,
        )

    core = lax.rem(gy, 2)
    own = ([send(gz, 0, n, 0, n) for n in range(PIECES)], [send(gz, 1, n, 1, n) for n in range(PIECES)])
    last = []
    for way in range(2):
        for n in range(REST):
            layers, first, size = stay(1 - way, n)
            piece = cc_o.at[gz, layers, pl.ds(first, size), :]
            last.append(
                pltpu.make_async_remote_copy(
                    piece, piece, (right_s, left_s)[way].at[2 * PIECES + n], (right_r, left_r)[way].at[2 * PIECES + n],
                    device_id={"gx": gx, "gy": gy, "gz": (right, left)[way]}, device_id_type=MESH,
                )
            )
    on = (
        [send(left, 0, n, 0, PIECES + n) for n in range(PIECES)],
        [send(right, 1, n, 1, PIECES + n) for n in range(PIECES)],
    )
    for n in range(PIECES):
        for way in range(2):
            apply(*place(way, n))
            own[way][n].start()

    new_rows = unpack_rows(jnp.concatenate(row_new, axis=0))
    for k in range(ROWS // 128):
        for l in range(LAYERS):
            rn_o[l : l + 1, 128 * k : 128 * (k + 1)] = new_rows[k][l]

    for copy in inverse:
        copy.wait_recv()
    for number in (1, 2):
        for pair in raws[number]:
            for copy in pair:
                copy.wait_recv()
    for i in range(1, nz):
        apply_raw(zs[i])
    for number in range(3):
        for pair in raws[number]:
            for copy in pair:
                copy.wait_send()
    for kind in range(2):
        apply(0, 2 * kind * PIECE, RAW)
    for n in range(PIECES):
        for way in range(2):
            own[way][n].wait_recv()
            on[way][n].start()

    @pl.when(core != LATE_CORE)
    def _():
        for copy in last:
            copy.start()

    for way in range(2):
        for n in range(PIECES):
            on[way][n].wait_recv()

    @pl.when(core != LATE_CORE)
    def _():
        for copy in last:
            copy.wait()

    for copy in exchange + inverse + own[0] + own[1] + on[0] + on[1]:
        copy.wait_send()
    pltpu.make_async_copy(all_x.at[pl.ds(0, len(others))], all_x.at[pl.ds(0, len(others))], all_s).wait()


def each(do):
    for way in range(2):
        for n in range(REST):
            do(way, n)


def columns_of(owner):
    return pl.ds(pl.multiple_of(owner * COLS, COLS), COLS)


def rest_kernel(nz, cc_v, after_h, late_o, right_s, right_r, left_s, left_r):
    gx, gy, gz = lax.axis_index("gx"), lax.axis_index("gy"), lax.axis_index("gz")
    right, left = lax.rem(gz + 1, nz), lax.rem(gz + nz - 1, nz)
    barrier = pltpu.get_barrier_semaphore()
    for z in (right, left):
        pl.semaphore_signal(barrier, inc=1, device_id={"gx": gx, "gy": gy, "gz": z}, device_id_type=MESH)
    pl.semaphore_wait(barrier, 2)

    def send(way, n):
        layers, first, size = stay(1 - way, n)
        return pltpu.make_async_remote_copy(
            cc_v.at[gz, layers, pl.ds(first, size), :], late_o.at[way, layers, pl.ds(2 * PIECE - size, size), :],
            (right_s, left_s)[way].at[n], (right_r, left_r)[way].at[n],
            device_id={"gx": gx, "gy": gy, "gz": (right, left)[way]}, device_id_type=MESH,
        )

    @pl.when(lax.rem(gy, 2) == LATE_CORE)
    def _():
        each(lambda way, n: send(way, n).start())
        each(lambda way, n: send(way, n).wait())


def write_kernel(nz, np_v, rn_v, cn_v, ap_v, cc_v, np_h, rn_h, cn_h, ap_h, cc_h, sem, part_sem):
    gy, gz = lax.axis_index("gy"), lax.axis_index("gz")
    right, left, across = lax.rem(gz + 1, nz), lax.rem(gz + nz - 1, nz), lax.rem(gz + 2, nz)
    copies = []

    def put(source, target):
        copies.append(pltpu.make_async_copy(source, target, sem.at[len(copies)]))
        copies[-1].start()

    def part(way, n):
        layers, first, size = stay(1 - way, n)
        rows = pl.ds(first, size)
        owner = (left, right)[way]
        return pltpu.make_async_copy(
            cc_v.at[owner, layers, rows, :], cc_h.at[layers, rows, columns_of(owner)], part_sem.at[way * REST + n]
        )

    early = lax.rem(gy, 2) != LATE_CORE

    @pl.when(early)
    def _():
        each(lambda way, n: part(way, n).start())

    for l in range(LAYERS):
        put(np_v.at[l], np_h.at[l])
        put(ap_v.at[l], ap_h.at[l])
        for owner in (gz, across):
            put(cc_v.at[owner, l], cc_h.at[l, :, columns_of(owner)])
        for kind, owner in ((0, left), (1, right)):
            rows = pl.ds(2 * kind * PIECE, 2 * PIECE)
            put(cc_v.at[owner, l, rows, :], cc_h.at[l, rows, columns_of(owner)])
    for kind, owner in ((1, left), (0, right)):
        rows = pl.ds(2 * kind * PIECE, RAW)
        put(cc_v.at[owner, 0, rows, :], cc_h.at[0, rows, columns_of(owner)])
    put(rn_v, rn_h)
    put(cn_v, cn_h)

    for copy in copies:
        copy.wait()

    @pl.when(early)
    def _():
        each(lambda way, n: part(way, n).wait())


def finish_kernel(nz, late_v, old_h, cc_h, part_sem):
    gy, gz = lax.axis_index("gy"), lax.axis_index("gz")
    right, left = lax.rem(gz + 1, nz), lax.rem(gz + nz - 1, nz)

    def part(way, n):
        layers, first, size = stay(1 - way, n)
        return pltpu.make_async_copy(
            late_v.at[way, layers, pl.ds(2 * PIECE - size, size), :],
            cc_h.at[layers, pl.ds(first, size), columns_of((left, right)[way])], part_sem.at[way * REST + n],
        )

    @pl.when(lax.rem(gy, 2) == LATE_CORE)
    def _():
        each(lambda way, n: part(way, n).start())
        each(lambda way, n: part(way, n).wait())


def solution(mesh):
    nx, ny, nz = (mesh.shape[a] for a in ("gx", "gy", "gz"))

    def body(params, grads, row_state, col_state):
        V = pltpu.VMEM
        sem = pltpu.SemaphoreType.DMA
        kept = pl.pallas_call(
            functools.partial(step_kernel, (nx, ny, nz)),
            out_shape=[
                V((LAYERS, ROWS, COLS), F32),
                V((LAYERS, ROWS), F32),
                V((LAYERS, COLS), F32),
                V((LAYERS, ROWS, COLS), F32),
                V((nz, LAYERS, ROWS, COLS), BF16),
            ],
            in_specs=[pl.BlockSpec(memory_space=pltpu.HBM)] * 4,
            out_specs=[pl.BlockSpec(memory_space=V)] * 5,
            scratch_shapes=[
                V((LAYERS, ROWS, COLS), BF16),
                V((LAYERS, ROWS), F32),
                V((LAYERS, COLS), F32),
                V((nz, 2, RAW, COLS), F32),
                V((nz, 2, RAW, COLS), BF16),
                V((nz, 1, COLS), F32),
                V((nz, LAYERS, 8, 128), F32),
                V((ny, LAYERS, 1, COLS), F32),
                V((nx * ny * nz, 1, 128), F32),
                V((LAYERS, 8, 128), F32),
                V((LAYERS, 1, COLS), F32),
                V((LAYERS, 1, COLS), F32),
                V((LAYERS, ROWS, 128), F32),
                pltpu.SemaphoreType.REGULAR, pltpu.SemaphoreType.REGULAR,
                sem((2 * LAYERS + 2,)),
                sem((nz - 1,)), sem((nz - 1,)),
                sem((ny - 1,)), sem((ny - 1,)),
                sem, sem,
                sem((nz - 1,)), sem((nz - 1,)),
                sem((6,)), sem((6,)), sem((6,)), sem((6,)),
                sem((2 * PIECES + REST,)), sem((2 * PIECES + REST,)),
                sem((2 * PIECES + REST,)), sem((2 * PIECES + REST,)),
            ],
            compiler_params=pltpu.CompilerParams(
                collective_id=0, has_side_effects=True, vmem_limit_bytes=16 * 2**20
            ),
        )(*[pltpu.with_memory_space_constraint(a, pltpu.HBM) for a in (params, grads, row_state, col_state)])
        new_params, row_new, col_new, applied, compute = pl.pallas_call(
            functools.partial(write_kernel, nz),
            out_shape=[
                jax.ShapeDtypeStruct((LAYERS, ROWS, COLS), F32),
                jax.ShapeDtypeStruct((LAYERS, ROWS), F32),
                jax.ShapeDtypeStruct((LAYERS, COLS), F32),
                jax.ShapeDtypeStruct((LAYERS, ROWS, COLS), F32),
                jax.ShapeDtypeStruct((LAYERS, ROWS, nz * COLS), BF16),
            ],
            in_specs=[pl.BlockSpec(memory_space=V)] * 5,
            out_specs=[pl.BlockSpec(memory_space=pltpu.HBM)] * 5,
            scratch_shapes=[sem((6 * LAYERS + 4,)), sem((2 * REST,))],
            compiler_params=pltpu.CompilerParams(vmem_limit_bytes=2**20),
        )(*kept)
        late = pl.pallas_call(
            functools.partial(rest_kernel, nz),
            out_shape=V((2, LAYERS, 2 * PIECE, COLS), BF16),
            in_specs=[pl.BlockSpec(memory_space=V), pl.BlockSpec(memory_space=pltpu.HBM)],
            out_specs=pl.BlockSpec(memory_space=V),
            scratch_shapes=[sem((REST,)), sem((REST,)), sem((REST,)), sem((REST,))],
            compiler_params=pltpu.CompilerParams(collective_id=1, has_side_effects=True, vmem_limit_bytes=2**20),
        )(kept[4], pltpu.with_memory_space_constraint(col_new, pltpu.HBM))
        compute = pl.pallas_call(
            functools.partial(finish_kernel, nz),
            out_shape=jax.ShapeDtypeStruct((LAYERS, ROWS, nz * COLS), BF16),
            in_specs=[pl.BlockSpec(memory_space=V), pl.BlockSpec(memory_space=pltpu.HBM)],
            out_specs=pl.BlockSpec(memory_space=pltpu.HBM),
            scratch_shapes=[sem((2 * REST,))],
            input_output_aliases={1: 0},
            compiler_params=pltpu.CompilerParams(vmem_limit_bytes=2**20),
        )(late, compute)
        return new_params, row_new, col_new, applied, compute

    return jax.shard_map(
        body,
        mesh=mesh,
        in_specs=(P("gx", "gy", "gz"), P("gx", "gy", "gz"), P("gx", "gy"), P("gx", "gz")),
        out_specs=(
            P("gx", "gy", "gz"),
            P("gx", "gy"),
            P("gx", "gz"),
            P("gx", "gy", "gz"),
            P("gx", "gy", None),
        ),
        check_vma=False,
    )
```

```python
import functools

import jax
import jax.numpy as jnp
from jax import lax
from jax.experimental import pallas as pl
from jax.experimental.pallas import tpu as pltpu
from jax.sharding import PartitionSpec as P

MESH = pl.DeviceIdType.MESH
F32 = jnp.float32
BF16 = jnp.bfloat16

decay_rate = 0.842
tiny_term = 1e-30
step_share = 0.01
clip_limit = 1.0

LAYERS = 3
ROWS = 896
COLS = 384
STEP = 112
RAW = 80
PIECE = ROWS // 4
PIECES = 2 * LAYERS
REST = 2
LATE_CORE = 1


def place(kind, n):
    first = (2 * kind + n % 2) * PIECE
    cut = RAW if n == 0 else 0
    return n // 2, first + cut, PIECE - cut


def stay(kind, n):
    cut = RAW if n == 0 else 0
    layers = pl.ds(0, 1) if n == 0 else pl.ds(1, LAYERS - 1)
    return layers, 2 * kind * PIECE + cut, 2 * PIECE - cut


def lanes(shape):
    return lax.broadcasted_iota(jnp.int32, shape, len(shape) - 1)


def advance(weights, gradient, inv_col, factor):
    scaled = gradient.astype(F32) * inv_col
    step = jnp.concatenate([scaled[:, 128 * k : 128 * k + 128] * factor for k in range(COLS // 128)], axis=1)
    return step, weights - step_share * step


def total(x):
    return jnp.sum(jnp.sum(x, axis=0, keepdims=True), axis=1, keepdims=True)


def lane_of(x, k):
    return jnp.sum(jnp.where(lanes(x.shape) == k, x, 0.0), axis=1, keepdims=True)


def pack_rows(lane_dense):
    sub = lax.broadcasted_iota(jnp.int32, (8, 128), 0)
    lane = lanes((8, 128))
    source = lax.broadcasted_iota(jnp.int32, (128, 128), 0)
    target = lanes((128, 128))
    packed = None
    for k in range(ROWS // 128):
        pick = (target == source // 8 + 16 * k).astype(F32)
        spread = [
            jnp.where(lane % 8 == sub, jnp.broadcast_to(lane_dense[l : l + 1, 128 * k : 128 * (k + 1)], (8, 128)), 0.0)
            for l in range(LAYERS)
        ]
        part = jnp.dot(
            jnp.concatenate(spread, axis=0), pick, preferred_element_type=F32, precision=lax.Precision.HIGHEST
        )
        packed = part if packed is None else packed + part
    return packed


def unpack_rows(packed):
    sub = lax.broadcasted_iota(jnp.int32, (8, 128), 0)
    lane = lanes((8, 128))
    source = lax.broadcasted_iota(jnp.int32, (128, 128), 0)
    target = lanes((128, 128))
    out = []
    for k in range(ROWS // 128):
        pick = (source == target // 8 + 16 * k).astype(F32)
        part = jnp.dot(packed, pick, preferred_element_type=F32, precision=lax.Precision.HIGHEST)
        out.append(
            [
                jnp.sum(jnp.where(lane % 8 == sub, part[8 * l : 8 * (l + 1)], 0.0), axis=0, keepdims=True)
                for l in range(LAYERS)
            ]
        )
    return out


def step_kernel(
    sizes,
    p_h, g_h, rs_h, cs_h,
    np_o, rn_o, cn_o, ap_o, cc_o,
    g_v, rs_v, cs_v, raw_p, raw_g, inv_x, row_x, col_x, all_x, row_inv, col_inv, col_w, rrb,
    told_line, told_plane, load_sem, row_s, row_r, col_s, col_r, all_s, all_r,
    inv_s, inv_r, raw_right_s, raw_right_r, raw_left_s, raw_left_r,
    right_s, right_r, left_s, left_r,
):
    nx, ny, nz = sizes
    gx, gy, gz = lax.axis_index("gx"), lax.axis_index("gy"), lax.axis_index("gz")
    right, left = lax.rem(gz + 1, nz), lax.rem(gz + nz - 1, nz)
    columns = COLS * nz
    rows_all = ROWS * ny

    loads = [pltpu.make_async_copy(g_h.at[l], g_v.at[l], load_sem.at[l]) for l in range(LAYERS)]
    loads += [
        pltpu.make_async_copy(rs_h, rs_v, load_sem.at[LAYERS]),
        pltpu.make_async_copy(cs_h, cs_v, load_sem.at[LAYERS + 1]),
    ]
    loads += [pltpu.make_async_copy(p_h.at[l], np_o.at[l], load_sem.at[LAYERS + 2 + l]) for l in range(LAYERS)]
    for load in loads:
        load.start()

    xs = [lax.rem(gx + i, nx) for i in range(nx)]
    ys = [lax.rem(gy + i, ny) for i in range(ny)]
    zs = [lax.rem(gz + i, nz) for i in range(nz)]
    barrier = pltpu.get_barrier_semaphore()

    def signal(sem, peers):
        for i, j, k in peers:
            pl.semaphore_signal(sem, inc=1, device_id={"gx": xs[i], "gy": ys[j], "gz": zs[k]}, device_id_type=MESH)

    line_x = [(i, 0, 0) for i in range(1, nx)]
    line_y = [(0, j, 0) for j in range(1, ny)]
    line_z = [(0, 0, k) for k in range(1, nz)]
    signal(barrier, line_x + line_y + line_z)

    lane = lanes((8, 128))

    def stats(l, carry):
        pltpu.make_async_copy(g_h.at[l], g_v.at[l], load_sem.at[l]).wait()
        packed = jnp.zeros((8, 128), F32)
        col_acc = jnp.zeros((8, COLS), F32)
        for t in range(ROWS // 16):
            x = g_v[l, 16 * t : 16 * t + 16, :].astype(F32)
            sq = x * x
            row = jnp.sum(sq[:, 0:128] + sq[:, 128:256] + sq[:, 256:384], axis=1, keepdims=True)
            packed = jnp.where(lane == 2 * t, row[0:8], packed)
            packed = jnp.where(lane == 2 * t + 1, row[8:16], packed)
            col_acc = col_acc + sq[0:8] + sq[8:16]
        row_x[gz, l] = packed
        col_x[gy, l] = jnp.sum(col_acc, axis=0, keepdims=True)
        return carry

    lax.fori_loop(0, LAYERS, stats, 0)

    pl.semaphore_wait(barrier, len(line_x + line_y + line_z))
    for load in loads[LAYERS + 2 :]:
        load.wait()
    exchange = []
    for i in range(1, nz):
        exchange.append(
            pltpu.make_async_remote_copy(
                row_x.at[gz], row_x.at[gz], row_s.at[i - 1], row_r.at[i - 1],
                device_id={"gx": gx, "gy": gy, "gz": zs[i]}, device_id_type=MESH,
            )
        )
    for i in range(1, ny):
        exchange.append(
            pltpu.make_async_remote_copy(
                col_x.at[gy], col_x.at[gy], col_s.at[i - 1], col_r.at[i - 1],
                device_id={"gx": gx, "gy": ys[i], "gz": gz}, device_id_type=MESH,
            )
        )
    for copy in exchange:
        copy.start()
    signal(told_line, line_z)

    def raw(way, number):
        kind = way if number != 1 else 1 - way
        owner = (left, right)[way] if number == 2 else gz
        rows = pl.ds(2 * kind * PIECE, RAW)
        sources = (raw_p.at[owner, kind], raw_g.at[owner, kind]) if number == 2 else (np_o.at[0, rows], g_v.at[0, rows])
        return [
            pltpu.make_async_remote_copy(
                source, target.at[owner, kind],
                (raw_right_s, raw_left_s)[way].at[2 * number + k], (raw_right_r, raw_left_r)[way].at[2 * number + k],
                device_id={"gx": gx, "gy": gy, "gz": (right, left)[way]}, device_id_type=MESH,
            )
            for k, (source, target) in enumerate(zip(sources, (raw_p, raw_g)))
        ]

    raws = [[raw(way, number) for way in range(2)] for number in range(3)]
    for pair in raws[0]:
        for copy in pair:
            copy.start()
    near = jnp.logical_and(gx == 0, gy // 2 == 0)

    @pl.when(near)
    def _():
        for pair in raws[1]:
            for copy in pair:
                copy.start()


    row1 = lanes((1, 128))

    def weigh(l, payload):
        def some(i, acc):
            for t in range(STEP // 8):
                w = np_o[l, pl.ds(pl.multiple_of(i * STEP + 8 * t, 8), 8), :]
                acc = acc + w * w
            for t in range(STEP // 16):
                rows = pl.ds(pl.multiple_of(i * STEP + 16 * t, 16), 16)
                x = g_v[l, rows, :].astype(F32)
                ap_o[l, rows, :] = x * x
            return acc

        squares = lax.fori_loop(0, ROWS // STEP, some, jnp.zeros((8, COLS), F32))
        return jnp.where(row1 == LAYERS + l, total(squares), payload)

    payload = lax.fori_loop(0, LAYERS, weigh, jnp.zeros((1, 128), F32))
    pl.semaphore_wait(told_line, len(line_z))
    signal(told_plane, line_y)
    loads[LAYERS].wait()
    loads[LAYERS + 1].wait()
    row_old = pack_rows(rs_v[...])

    for copy in exchange[: nz - 1]:
        copy.wait_recv()
    row_new = []
    for l in range(LAYERS):
        row_sum = row_x[0, l]
        for k in range(1, nz):
            row_sum = row_sum + row_x[k, l]
        new = decay_rate * row_old[8 * l : 8 * l + 8] + (1.0 - decay_rate) * (row_sum / columns + tiny_term)
        row_new.append(new)
        row_inv[l] = lax.rsqrt(new)
        payload = jnp.where(row1 == 2 * LAYERS + l, total(jnp.where(lane < ROWS // 8, new, 0.0)), payload)

    def updates(l, carry):
        acc = [jnp.zeros((8, 128), F32)] * (COLS // 128)
        inv_packed = row_inv[l]
        for t in range(ROWS // 8):
            inv = jnp.sum(jnp.where(lane == t, inv_packed, 0.0), axis=1, keepdims=True)
            inv = jnp.broadcast_to(inv, (8, 128))
            rrb[l, 8 * t : 8 * t + 8, :] = inv
            inv = inv * inv
            for k in range(COLS // 128):
                acc[k] = acc[k] + ap_o[l, 8 * t : 8 * t + 8, 128 * k : 128 * k + 128] * inv
        col_w[l] = jnp.sum(jnp.concatenate(acc, axis=1), axis=0, keepdims=True)
        return carry

    lax.fori_loop(0, LAYERS, updates, 0)
    for copy in exchange[nz - 1 :]:
        copy.wait_recv()
    for l in range(LAYERS):
        col_sum = col_x[0, l]
        for k in range(1, ny):
            col_sum = col_sum + col_x[k, l]
        new = decay_rate * cs_v[l : l + 1, :] + (1.0 - decay_rate) * (col_sum / rows_all + tiny_term)
        cn_o[l : l + 1, :] = new
        inv = lax.rsqrt(new)
        col_inv[l] = inv
        payload = jnp.where(row1 == l, total(col_w[l] * (inv * inv)), payload)
    inv_x[gz] = col_inv[0]
    inverse = [
        pltpu.make_async_remote_copy(
            inv_x.at[gz], inv_x.at[gz], inv_s.at[i - 1], inv_r.at[i - 1],
            device_id={"gx": gx, "gy": gy, "gz": zs[i]}, device_id_type=MESH,
        )
        for i in range(1, nz)
    ]

    all_x[(gx * ny + gy) * nz + gz] = payload
    pl.semaphore_wait(told_plane, len(line_y))
    mine = all_x.at[(gx * ny + gy) * nz + gz]

    def far(at):
        return sum(min(a, n - a) for a, n in zip((at[0], at[1] // 2, at[2]), (nx, ny // 2, nz)))

    others = [(i, j, k) for i in range(nx) for j in range(ny) for k in range(nz) if i or j or k]
    for i, j, k in sorted(others, key=far, reverse=True):
        pltpu.make_async_remote_copy(
            mine, mine, all_s, all_r,
            device_id={"gx": xs[i], "gy": ys[j], "gz": zs[k]}, device_id_type=MESH,
        ).start()
    for copy in inverse:
        copy.start()
    @pl.when(jnp.logical_not(near))
    def _():
        for pair in raws[1]:
            for copy in pair:
                copy.start()

    for way in range(2):
        for copy in raws[0][way]:
            copy.wait_recv()
        for copy in raws[2][way]:
            copy.start()
    pltpu.make_async_copy(all_x.at[pl.ds(0, len(others))], all_x.at[pl.ds(0, len(others))], all_r).wait()
    everything = jnp.zeros((1, 1), F32)
    scale = [jnp.zeros((1, 1), F32)] * LAYERS
    for i in range(nx):
        sums = jnp.sum(all_x[i * ny * nz : (i + 1) * ny * nz], axis=0)
        for l in range(LAYERS):
            mean_row = lane_of(sums, 2 * LAYERS + l) / (nz * rows_all)
            everything = everything + mean_row * lane_of(sums, l)
            root = jnp.sqrt(lane_of(sums, LAYERS + l) / (rows_all * columns)) * jnp.sqrt(mean_row)
            scale[l] = jnp.where(gx == i, root, scale[l])
    entries = float(nx * LAYERS * rows_all * columns)
    clip = jnp.maximum(1.0, jnp.sqrt(everything / entries) / clip_limit)
    scale = [one / clip for one in scale]

    def apply(l, first, size):
        inv_col = col_inv[l]

        tiles = size // 16
        at_once = max(k for k in range(1, 12) if tiles % k == 0)

        def some(i, carry):
            for t in range(at_once):
                rows = pl.ds(pl.multiple_of(first + (i * at_once + t) * 16, 16), 16)
                step, new = advance(np_o[l, rows, :], g_v[l, rows, :], inv_col, rrb[l, rows, :] * scale[l])
                ap_o[l, rows, :] = step
                np_o[l, rows, :] = new
                cc_o[gz, l, rows, :] = new.astype(BF16)
            return carry

        lax.fori_loop(0, tiles // at_once, some, 0)

    def apply_raw(owner):
        inv_col = inv_x[owner]
        for kind in range(2):
            for t in range(RAW // 16):
                rows = pl.ds(2 * kind * PIECE + 16 * t, 16)
                some = pl.ds(16 * t, 16)
                _, new = advance(
                    raw_p[owner, kind, some, :], raw_g[owner, kind, some, :], inv_col, rrb[0, rows, :] * scale[0]
                )
                cc_o[owner, 0, rows, :] = new.astype(BF16)

    def send(owner, kind, n, way, number):
        l, first, size = place(kind, n)
        piece = cc_o.at[owner, l, pl.ds(first, size), :]
        return pltpu.make_async_remote_copy(
            piece, piece, (right_s, left_s)[way].at[number], (right_r, left_r)[way].at[number],
            device_id={"gx": gx, "gy": gy, "gz": (right, left)[way]}, device_id_type=MESH,
        )

    core = lax.rem(gy, 2)
    own = ([send(gz, 0, n, 0, n) for n in range(PIECES)], [send(gz, 1, n, 1, n) for n in range(PIECES)])
    last = []
    for way in range(2):
        for n in range(REST):
            layers, first, size = stay(1 - way, n)
            piece = cc_o.at[gz, layers, pl.ds(first, size), :]
            last.append(
                pltpu.make_async_remote_copy(
                    piece, piece, (right_s, left_s)[way].at[2 * PIECES + n], (right_r, left_r)[way].at[2 * PIECES + n],
                    device_id={"gx": gx, "gy": gy, "gz": (right, left)[way]}, device_id_type=MESH,
                )
            )
    on = (
        [send(left, 0, n, 0, PIECES + n) for n in range(PIECES)],
        [send(right, 1, n, 1, PIECES + n) for n in range(PIECES)],
    )
    for n in range(PIECES):
        for way in range(2):
            apply(*place(way, n))
            own[way][n].start()

    new_rows = unpack_rows(jnp.concatenate(row_new, axis=0))
    for k in range(ROWS // 128):
        for l in range(LAYERS):
            rn_o[l : l + 1, 128 * k : 128 * (k + 1)] = new_rows[k][l]

    for copy in inverse:
        copy.wait_recv()
    for number in (1, 2):
        for pair in raws[number]:
            for copy in pair:
                copy.wait_recv()
    for i in range(1, nz):
        apply_raw(zs[i])
    for number in range(3):
        for pair in raws[number]:
            for copy in pair:
                copy.wait_send()
    for kind in range(2):
        apply(0, 2 * kind * PIECE, RAW)
    for n in range(PIECES):
        for way in range(2):
            own[way][n].wait_recv()
            on[way][n].start()

    @pl.when(core != LATE_CORE)
    def _():
        for copy in last:
            copy.start()

    for way in range(2):
        for n in range(PIECES):
            on[way][n].wait_recv()

    @pl.when(core != LATE_CORE)
    def _():
        for copy in last:
            copy.wait()

    for copy in exchange + inverse + own[0] + own[1] + on[0] + on[1]:
        copy.wait_send()
    pltpu.make_async_copy(all_x.at[pl.ds(0, len(others))], all_x.at[pl.ds(0, len(others))], all_s).wait()


def each(do):
    for way in range(2):
        for n in range(REST):
            do(way, n)


def columns_of(owner):
    return pl.ds(pl.multiple_of(owner * COLS, COLS), COLS)


def rest_kernel(nz, cc_v, after_h, late_o, right_s, right_r, left_s, left_r):
    gx, gy, gz = lax.axis_index("gx"), lax.axis_index("gy"), lax.axis_index("gz")
    right, left = lax.rem(gz + 1, nz), lax.rem(gz + nz - 1, nz)
    barrier = pltpu.get_barrier_semaphore()
    for z in (right, left):
        pl.semaphore_signal(barrier, inc=1, device_id={"gx": gx, "gy": gy, "gz": z}, device_id_type=MESH)
    pl.semaphore_wait(barrier, 2)

    def send(way, n):
        layers, first, size = stay(1 - way, n)
        return pltpu.make_async_remote_copy(
            cc_v.at[gz, layers, pl.ds(first, size), :], late_o.at[way, layers, pl.ds(2 * PIECE - size, size), :],
            (right_s, left_s)[way].at[n], (right_r, left_r)[way].at[n],
            device_id={"gx": gx, "gy": gy, "gz": (right, left)[way]}, device_id_type=MESH,
        )

    @pl.when(lax.rem(gy, 2) == LATE_CORE)
    def _():
        each(lambda way, n: send(way, n).start())
        each(lambda way, n: send(way, n).wait())


def write_kernel(nz, np_v, rn_v, cn_v, ap_v, cc_v, np_h, rn_h, cn_h, ap_h, cc_h, sem, part_sem):
    gy, gz = lax.axis_index("gy"), lax.axis_index("gz")
    right, left, across = lax.rem(gz + 1, nz), lax.rem(gz + nz - 1, nz), lax.rem(gz + 2, nz)
    copies = []

    def put(source, target):
        copies.append(pltpu.make_async_copy(source, target, sem.at[len(copies)]))
        copies[-1].start()

    def part(way, n):
        layers, first, size = stay(1 - way, n)
        rows = pl.ds(first, size)
        owner = (left, right)[way]
        return pltpu.make_async_copy(
            cc_v.at[owner, layers, rows, :], cc_h.at[layers, rows, columns_of(owner)], part_sem.at[way * REST + n]
        )

    early = lax.rem(gy, 2) != LATE_CORE

    @pl.when(early)
    def _():
        each(lambda way, n: part(way, n).start())

    for l in range(LAYERS):
        put(np_v.at[l], np_h.at[l])
        put(ap_v.at[l], ap_h.at[l])
        for owner in (gz, across):
            put(cc_v.at[owner, l], cc_h.at[l, :, columns_of(owner)])
        for kind, owner in ((0, left), (1, right)):
            rows = pl.ds(2 * kind * PIECE, 2 * PIECE)
            put(cc_v.at[owner, l, rows, :], cc_h.at[l, rows, columns_of(owner)])
    for kind, owner in ((1, left), (0, right)):
        rows = pl.ds(2 * kind * PIECE, RAW)
        put(cc_v.at[owner, 0, rows, :], cc_h.at[0, rows, columns_of(owner)])
    put(rn_v, rn_h)
    put(cn_v, cn_h)

    for copy in copies:
        copy.wait()

    @pl.when(early)
    def _():
        each(lambda way, n: part(way, n).wait())


def finish_kernel(nz, late_v, old_h, cc_h, part_sem):
    gy, gz = lax.axis_index("gy"), lax.axis_index("gz")
    right, left = lax.rem(gz + 1, nz), lax.rem(gz + nz - 1, nz)

    def part(way, n):
        layers, first, size = stay(1 - way, n)
        return pltpu.make_async_copy(
            late_v.at[way, layers, pl.ds(2 * PIECE - size, size), :],
            cc_h.at[layers, pl.ds(first, size), columns_of((left, right)[way])], part_sem.at[way * REST + n],
        )

    @pl.when(lax.rem(gy, 2) == LATE_CORE)
    def _():
        each(lambda way, n: part(way, n).start())
        each(lambda way, n: part(way, n).wait())


def solution(mesh):
    nx, ny, nz = (mesh.shape[a] for a in ("gx", "gy", "gz"))

    def body(params, grads, row_state, col_state):
        V = pltpu.VMEM
        sem = pltpu.SemaphoreType.DMA
        kept = pl.pallas_call(
            functools.partial(step_kernel, (nx, ny, nz)),
            out_shape=[
                V((LAYERS, ROWS, COLS), F32),
                V((LAYERS, ROWS), F32),
                V((LAYERS, COLS), F32),
                V((LAYERS, ROWS, COLS), F32),
                V((nz, LAYERS, ROWS, COLS), BF16),
            ],
            in_specs=[pl.BlockSpec(memory_space=pltpu.HBM)] * 4,
            out_specs=[pl.BlockSpec(memory_space=V)] * 5,
            scratch_shapes=[
                V((LAYERS, ROWS, COLS), BF16),
                V((LAYERS, ROWS), F32),
                V((LAYERS, COLS), F32),
                V((nz, 2, RAW, COLS), F32),
                V((nz, 2, RAW, COLS), BF16),
                V((nz, 1, COLS), F32),
                V((nz, LAYERS, 8, 128), F32),
                V((ny, LAYERS, 1, COLS), F32),
                V((nx * ny * nz, 1, 128), F32),
                V((LAYERS, 8, 128), F32),
                V((LAYERS, 1, COLS), F32),
                V((LAYERS, 1, COLS), F32),
                V((LAYERS, ROWS, 128), F32),
                pltpu.SemaphoreType.REGULAR, pltpu.SemaphoreType.REGULAR,
                sem((2 * LAYERS + 2,)),
                sem((nz - 1,)), sem((nz - 1,)),
                sem((ny - 1,)), sem((ny - 1,)),
                sem, sem,
                sem((nz - 1,)), sem((nz - 1,)),
                sem((6,)), sem((6,)), sem((6,)), sem((6,)),
                sem((2 * PIECES + REST,)), sem((2 * PIECES + REST,)),
                sem((2 * PIECES + REST,)), sem((2 * PIECES + REST,)),
            ],
            compiler_params=pltpu.CompilerParams(
                collective_id=0, has_side_effects=True, vmem_limit_bytes=16 * 2**20
            ),
        )(*[pltpu.with_memory_space_constraint(a, pltpu.HBM) for a in (params, grads, row_state, col_state)])
        new_params, row_new, col_new, applied, compute = pl.pallas_call(
            functools.partial(write_kernel, nz),
            out_shape=[
                jax.ShapeDtypeStruct((LAYERS, ROWS, COLS), F32),
                jax.ShapeDtypeStruct((LAYERS, ROWS), F32),
                jax.ShapeDtypeStruct((LAYERS, COLS), F32),
                jax.ShapeDtypeStruct((LAYERS, ROWS, COLS), F32),
                jax.ShapeDtypeStruct((LAYERS, ROWS, nz * COLS), BF16),
            ],
            in_specs=[pl.BlockSpec(memory_space=V)] * 5,
            out_specs=[pl.BlockSpec(memory_space=pltpu.HBM)] * 5,
            scratch_shapes=[sem((6 * LAYERS + 4,)), sem((2 * REST,))],
            compiler_params=pltpu.CompilerParams(vmem_limit_bytes=2**20),
        )(*kept)
        late = pl.pallas_call(
            functools.partial(rest_kernel, nz),
            out_shape=V((2, LAYERS, 2 * PIECE, COLS), BF16),
            in_specs=[pl.BlockSpec(memory_space=V), pl.BlockSpec(memory_space=pltpu.HBM)],
            out_specs=pl.BlockSpec(memory_space=V),
            scratch_shapes=[sem((REST,)), sem((REST,)), sem((REST,)), sem((REST,))],
            compiler_params=pltpu.CompilerParams(collective_id=1, has_side_effects=True, vmem_limit_bytes=2**20),
        )(kept[4], pltpu.with_memory_space_constraint(col_new, pltpu.HBM))
        compute = pl.pallas_call(
            functools.partial(finish_kernel, nz),
            out_shape=jax.ShapeDtypeStruct((LAYERS, ROWS, nz * COLS), BF16),
            in_specs=[pl.BlockSpec(memory_space=V), pl.BlockSpec(memory_space=pltpu.HBM)],
            out_specs=pl.BlockSpec(memory_space=pltpu.HBM),
            scratch_shapes=[sem((2 * REST,))],
            input_output_aliases={1: 0},
            compiler_params=pltpu.CompilerParams(vmem_limit_bytes=2**20),
        )(late, compute)
        return new_params, row_new, col_new, applied, compute

    return jax.shard_map(
        body,
        mesh=mesh,
        in_specs=(P("gx", "gy", "gz"), P("gx", "gy", "gz"), P("gx", "gy"), P("gx", "gz")),
        out_specs=(
            P("gx", "gy", "gz"),
            P("gx", "gy"),
            P("gx", "gz"),
            P("gx", "gy", "gz"),
            P("gx", "gy", None),
        ),
        check_vma=False,
    )
```
